32 devices in a mesh: dp: 16 (over z, y, x), head: 2 (over core).
Axes of the slice: x: 2, y: 2, z: 4, core: 2. Of those that a mesh axis runs over, the one named last changes fastest.
Arguments:
- hidden: bfloat16 [64, 512, 3584], P(('dp', 'head')), may hold values from -6 to 6
- head_proj: bfloat16 [4, 3584, 128], P('head'), may hold values from -0.09375 to 0.09375
- head_out: bfloat16 [4, 128], P('head'), may hold values from -0.8984375 to 0.8984375
- head_ratio: int32 [4], replicated, may hold values from 2 to 7
- group_of: int32 [64], replicated, may hold values from 0 to 3, as said below
- lengths: int32 [64], P(('dp', 'head')), may hold values from 1 to 512
- token_mask: int32 [64, 512], P(('dp', 'head')), may hold values 0 or 1
Outputs:
- advantages: float32 [64, 512], P(('dp', 'head'))
The draws below stay inside these ranges and needn't reach their ends.
Inputs may be any that keep to these rules, and one draw needn't show every extreme that they name: `group_of`: every one of the 4 groups holds exactly 16 rollouts.
All inputs are finite; a program needn't handle non-finite values. No bound on the sum of `token_mask` on one device may be relied on, other than what follows from the above.
Results may differ from the reference program's by a relative error of at most 0.0026.
Values may be sent and summed in bfloat16 or wider, within the bound.
A program may use at most 64 MiB of HBM per device.

```python
import jax
import jax.numpy as jnp
from jax import lax

D = 3584
HEADS = 4
RANK = 128
GROUP = 16
LEN = 512
ROLL = 64
GROUPS = 4


def draw_group_of(key, part):
    order = jax.random.permutation(key, ROLL)
    return (order // GROUP).astype(jnp.int32)


def place_ends(result, own_key, smallest, high):
    extent = result.shape
    spot = [jax.random.randint(jax.random.fold_in(own_key, axis), (), 0, extent[axis]) for axis in range(len(extent))]
    result = result.at[tuple(spot)].set(smallest)
    longest = extent.index(max(extent))
    spot[longest] = (spot[longest] + 1) % extent[longest]
    return result.at[tuple(spot)].set(high)


def block_scale(rng, extent, split, least, top_value):
    def one(dim, blocks):
        draws = jax.random.uniform(jax.random.fold_in(jax.random.fold_in(rng, 6), dim), (blocks,), jnp.float32, least / len(split), top_value / len(split))
        return jnp.repeat(jnp.exp(draws), extent[dim] // blocks).reshape((-1,) + (1,) * (len(extent) - dim - 1))

    loudness = one(*split[0])
    for cut in split[1:]:
        loudness = loudness * one(*cut)
    return loudness


def gaussian(stream_key, extent, width, reach, pieces=(), held_as=jnp.bfloat16):
    result = jax.random.normal(stream_key, extent, jnp.float32) * width
    if len(pieces) > 0:
        result = block_scale(stream_key, extent, pieces, -0.22, 0.18) * result
    return jnp.clip(result, min=-reach, max=reach).astype(held_as)


def setup_inputs(seed: int = 0) -> dict:
    key_list = jax.random.split(jax.random.key(seed), 8)
    hidden = gaussian(key_list[0], (ROLL, LEN, D), 1.0, 6.0, ((0, 32),))
    head_proj = gaussian(key_list[1], (HEADS, D, RANK), D ** -0.5, 0.09375, ((0, 2),))
    head_out = gaussian(key_list[2], (HEADS, RANK), 0.15, 0.8984375, ((0, 2),))
    head_ratio = place_ends(jax.random.randint(key_list[3], (HEADS,), 2, 8), jax.random.fold_in(key_list[3], 1), 2, 7).astype(jnp.int32)
    group_of = draw_group_of(jax.random.fold_in(key_list[7], 71), 0)
    lengths = place_ends(jax.random.randint(key_list[5], (ROLL,), 1, LEN + 1), jax.random.fold_in(key_list[5], 1), 1, LEN).astype(jnp.int32)
    token_mask = place_ends((jax.random.randint(key_list[6], (ROLL, LEN), 0, 4) < 3).astype(jnp.int32), jax.random.fold_in(key_list[6], 1), 0, 1)
    return dict(hidden=hidden, head_proj=head_proj, head_out=head_out, head_ratio=head_ratio, group_of=group_of, lengths=lengths, token_mask=token_mask)


token_weight = 0.5
gap_weight = 0.5
clip_limit = 2.0
var_offset = 0.04

def head_mixture(head_ratio):
    ratios = head_ratio.astype(jnp.float32)
    return ratios / jnp.sum(ratios)

def reference(hidden, head_proj, head_out, head_ratio, group_of, lengths, token_mask):
    mixture = head_mixture(head_ratio)
    proj_wide = head_proj.astype(jnp.float32)
    out_wide = head_out.astype(jnp.float32)

    def rollout_score(states):
        hidden_pre = jnp.einsum('ld,hdr->hlr', states.astype(jnp.float32), proj_wide)
        active = jnp.tanh(hidden_pre).astype(jnp.bfloat16)
        active = lax.optimization_barrier(active)
        scores = jnp.einsum('hlr,hr->hl', active.astype(jnp.float32), out_wide)
        return lax.optimization_barrier(jnp.sum(mixture[:, None] * scores, axis=0))
    combined = lax.map(rollout_score, hidden)
    positions = jnp.arange(LEN)
    last_mark = positions[None, :] == (lengths - 1)[:, None]
    reward = lax.optimization_barrier(jnp.sum(jnp.where(last_mark, combined, 0.0), axis=1))
    member = (group_of[:, None] == jnp.arange(GROUPS)[None, :]).astype(jnp.float32)
    group_mean = lax.optimization_barrier(jnp.sum(member * reward[:, None], axis=0)) / GROUP
    mean_rows = lax.optimization_barrier(jnp.sum(member * group_mean[None, :], axis=1))
    deviation = reward - mean_rows
    group_var = lax.optimization_barrier(jnp.sum(member * (deviation * deviation)[:, None], axis=0)) / GROUP
    group_best = lax.optimization_barrier(jnp.max(jnp.where(member > 0, reward[:, None], -jnp.inf), axis=0))
    var_rows = lax.optimization_barrier(jnp.sum(member * group_var[None, :], axis=1))
    best_rows = lax.optimization_barrier(jnp.sum(member * group_best[None, :], axis=1))
    shaped = (deviation / jnp.sqrt(var_rows + var_offset))[:, None] + token_weight * combined - gap_weight * (best_rows - reward)[:, None]
    valid_mask = (positions[None, :] < lengths[:, None]) & (token_mask == 1)
    return jnp.where(valid_mask, jnp.clip(shaped, -clip_limit, clip_limit), 0.0)
```

```python
import functools

import jax
import jax.numpy as jnp
from jax import lax
from jax.experimental import pallas as pl
from jax.experimental.pallas import tpu as pltpu
from jax.sharding import PartitionSpec as P

GROUP = 16
MESH = pl.DeviceIdType.MESH

token_weight = 0.5
gap_weight = 0.5
clip_limit = 2.0
var_offset = 0.04

DEPTH_PIECES = 2
PACK = 16


def kernel(
    chips,
    hidden, proj, readout, ratio, groups, lens, mask, out,
    rows_all, w_own, w_other, out_own, out_other, acc, comb, ends, msg, slots,
    ratio_s, groups_s, lens_s, groups_v, mask_v,
    row_sem, w_sem, small_sem, pair_send, pair_recv, all_send, all_recv,
):
    chip, core = lax.axis_index("dp"), lax.axis_index("head")
    width = hidden.shape[2]
    count, seq = mask.shape
    heads, _, rank = proj.shape
    devices = 2 * chips
    me = 2 * chip + core
    total_rows = count * seq
    depth = width // DEPTH_PIECES
    lanes = msg.shape[1]

    loads = [pltpu.make_async_copy(lens, lens_s, small_sem.at[0])]
    loads.append(pltpu.make_async_copy(ratio, ratio_s, small_sem.at[1]))
    loads.append(pltpu.make_async_copy(groups, groups_s, small_sem.at[2]))
    loads.append(pltpu.make_async_copy(readout, out_own, small_sem.at[3]))
    loads.append(pltpu.make_async_copy(groups, groups_v.at[0], small_sem.at[4]))
    loads.append(pltpu.make_async_copy(mask, mask_v, small_sem.at[5]))
    w_loads = [
        pltpu.make_async_copy(proj.at[k], w_own.at[:, pl.ds(k * rank, rank)], w_sem.at[k])
        for k in range(heads)
    ]
    cuts = [pl.ds(d * depth, depth) for d in range(DEPTH_PIECES)]
    h_loads = [
        pltpu.make_async_copy(hidden.at[:, :, cuts[d]], rows_all.at[:, :, cuts[d]], row_sem.at[d])
        for d in range(DEPTH_PIECES)
    ]
    for copy in loads[:1] + h_loads + w_loads + loads[1:]:
        copy.start()

    barrier = pltpu.get_barrier_semaphore()

    def each_other(act):
        def both(step, _):
            there = lax.rem(chip + step, chips)
            act((there, core))
            act((there, 1 - core))
            return 0

        if chips <= 16:
            for step in range(1, chips):
                both(step, 0)
        else:
            lax.fori_loop(1, chips, both, 0)
        act((chip, 1 - core))

    each_other(
        lambda place: pl.semaphore_signal(barrier, inc=1, device_id=place, device_id_type=MESH)
    )

    for copy in loads[:1] + h_loads:
        copy.wait()

    sub = lax.broadcasted_iota(jnp.int32, (PACK, width), 0)
    picked = jnp.zeros((PACK, width), jnp.float32)
    for r in range(count):
        last = lens_s[r] - 1
        block = rows_all[r * (seq // PACK) + lax.div(last, PACK)].astype(jnp.float32)
        row = jnp.sum(jnp.where(sub == lax.rem(last, PACK), block, 0.0), axis=0, keepdims=True)
        picked = jnp.where(sub == r, jnp.broadcast_to(row, (PACK, width)), picked)
    ends[pl.ds(0, PACK), :] = picked.astype(jnp.bfloat16)

    pl.semaphore_wait(barrier, devices - 1)

    def to_pair(src, dst, k):
        return pltpu.make_async_remote_copy(
            src_ref=src, dst_ref=dst, send_sem=pair_send.at[k], recv_sem=pair_recv.at[k],
            device_id=(chip, 1 - core), device_id_type=MESH,
        )

    send_ends = to_pair(ends.at[pl.ds(0, PACK)], ends.at[pl.ds(PACK, PACK)], 0)
    send_out = to_pair(out_own, out_other, 1)
    send_w = [
        to_pair(w_own.at[cuts[d]], w_other.at[cuts[d]], 2 + d)
        for d in range(DEPTH_PIECES)
    ]
    send_ends.start()
    for copy in w_loads + loads[1:]:
        copy.wait()
    send_out.start()
    send_w[0].start()

    weights = [ratio_s[k].astype(jnp.float32) for k in range(2 * heads)]
    weight_sum = sum(weights[1:], weights[0])
    own_mix = [
        ratio_s[core * heads + k].astype(jnp.float32) / weight_sum for k in range(heads)
    ]
    other_mix = [
        ratio_s[(1 - core) * heads + k].astype(jnp.float32) / weight_sum for k in range(heads)
    ]

    def reader(values):
        wide = values[...].astype(jnp.float32)
        line = lax.broadcasted_iota(jnp.int32, (8, rank), 0)
        parts = [
            jnp.where(line == k, jnp.broadcast_to(wide[k : k + 1], (8, rank)), 0.0)
            for k in range(heads)
        ]
        return jnp.concatenate(parts, axis=1).astype(jnp.bfloat16)

    def scores(inner, lhs, mix):
        active = jnp.tanh(inner).astype(jnp.bfloat16)
        per_head = lax.dot_general(
            lhs, active, (((1,), (1,)), ((), ())), preferred_element_type=jnp.float32
        )
        line = mix[0] * per_head[0:1]
        for k in range(1, heads):
            line = line + mix[k] * per_head[k : k + 1]
        return line

    own_lhs = reader(out_own)

    def partial(values, d):
        rows = rows_all[:, :, cuts[d]].reshape(total_rows, depth)
        return jnp.dot(rows, values[cuts[d], :], preferred_element_type=jnp.float32)

    def add_partial(values, d):
        inner = partial(values, d)
        if d > 0:
            inner = acc[...] + inner
        if d < DEPTH_PIECES - 1:
            acc[...] = inner
        return inner

    add_partial(w_own, 0)
    send_ends.wait_recv()

    inner = jnp.dot(ends[...], w_own[...], preferred_element_type=jnp.float32)
    active = jnp.tanh(inner).astype(jnp.bfloat16).astype(jnp.float32)
    wide = out_own[...].astype(jnp.float32)
    scale = jnp.concatenate([own_mix[k] * wide[k : k + 1] for k in range(heads)], axis=1)
    part = jnp.sum(active * scale, axis=1, keepdims=True)
    line = lax.broadcasted_iota(jnp.int32, (2 * PACK, lanes), 0)
    lane = lax.broadcasted_iota(jnp.int32, (2 * PACK, lanes), 1)
    mine = (line < count) & (lane == me * count + line)
    theirs = (line >= PACK) & (line < PACK + count) & (
        lane == (4 * chip + 1 - me) * count + line - PACK
    )
    note = jnp.sum(jnp.where(mine | theirs, part, 0.0), axis=0, keepdims=True)
    msg[...] = note
    slots[me] = note

    each_other(
        lambda place: pltpu.make_async_remote_copy(
            src_ref=msg, dst_ref=slots.at[me], send_sem=all_send, recv_sem=all_recv,
            device_id=place, device_id_type=MESH,
        ).start()
    )
    for copy in send_w[1:]:
        copy.start()

    for d in range(1, DEPTH_PIECES):
        inner = add_partial(w_own, d)
    comb[...] = scores(inner, own_lhs, own_mix)

    send_out.wait_recv()
    other_lhs = reader(out_other)
    for d in range(DEPTH_PIECES):
        send_w[d].wait_recv()
        inner = add_partial(w_other, d)
    comb[...] = comb[...] + scores(inner, other_lhs, other_mix)

    rest = slots.at[pl.ds(0, devices - 1)]
    pltpu.make_async_copy(rest, rest, all_recv).wait()

    reward = jnp.sum(slots[...], axis=0)[:, : groups_v.shape[1]]
    labels = groups_v[...]
    shape = (count, reward.shape[1])
    rollout = lax.broadcasted_iota(jnp.int32, shape, 0)
    lane_of = lax.broadcasted_iota(jnp.int32, shape, 1)
    wide = jnp.broadcast_to(reward, shape)
    group = jnp.zeros(shape, jnp.int32)
    length = jnp.zeros((count, seq), jnp.int32)
    line = lax.broadcasted_iota(jnp.int32, (count, seq), 0)
    for r in range(count):
        group = jnp.where(rollout == r, groups_s[me * count + r], group)
        length = jnp.where(line == r, lens_s[r], length)
    member = jnp.broadcast_to(labels, shape) == group
    own = jnp.sum(jnp.where(lane_of == me * count + rollout, wide, 0.0), axis=1, keepdims=True)
    mean = jnp.sum(jnp.where(member, wide, 0.0), axis=1, keepdims=True) / GROUP
    gap = wide - mean
    var = jnp.sum(jnp.where(member, gap * gap, 0.0), axis=1, keepdims=True) / GROUP
    best = jnp.max(jnp.where(member, wide, -jnp.inf), axis=1, keepdims=True)
    base = (own - mean) / jnp.sqrt(var + var_offset) - gap_weight * (best - own)
    shaped = base + token_weight * jnp.concatenate(
        [comb[:, pl.ds(r * seq, seq)] for r in range(count)], axis=0
    )
    place = lax.broadcasted_iota(jnp.int32, (count, seq), 1)
    valid = (place < length) & (mask_v[...] == 1)
    out[...] = jnp.where(valid, jnp.clip(shaped, -clip_limit, clip_limit), 0.0)

    send_ends.wait_send()
    send_out.wait_send()
    for copy in send_w:
        copy.wait_send()
    pltpu.make_async_copy(rest, rest, all_send).wait()


def solution(mesh):
    chips = mesh.shape["dp"]

    def on_device(hidden, head_proj, head_out, head_ratio, group_of, lengths, token_mask):
        count, seq, width = hidden.shape
        heads, _, rank = head_proj.shape
        everyone = group_of.shape[0]
        lanes = -(-everyone // 128) * 128
        hbm = pl.BlockSpec(memory_space=pltpu.HBM)
        bf16, f32, i32 = jnp.bfloat16, jnp.float32, jnp.int32
        return pl.pallas_call(
            functools.partial(kernel, chips),
            out_shape=pltpu.VMEM((count, seq), f32),
            in_specs=[hbm] * 7,
            out_specs=pl.BlockSpec(memory_space=pltpu.VMEM),
            scratch_shapes=[
                pltpu.VMEM((count * seq // PACK, PACK, width), bf16),
                pltpu.VMEM((width, heads * rank), bf16),
                pltpu.VMEM((width, heads * rank), bf16),
                pltpu.VMEM((heads, rank), bf16),
                pltpu.VMEM((heads, rank), bf16),
                pltpu.VMEM((count * seq, heads * rank), f32),
                pltpu.VMEM((1, count * seq), f32),
                pltpu.VMEM((2 * PACK, width), bf16),
                pltpu.VMEM((1, lanes), f32),
                pltpu.VMEM((2 * chips, 1, lanes), f32),
                pltpu.SMEM(head_ratio.shape, i32),
                pltpu.SMEM(group_of.shape, i32),
                pltpu.SMEM(lengths.shape, i32),
                pltpu.VMEM((1, everyone), i32),
                pltpu.VMEM((count, seq), i32),
                pltpu.SemaphoreType.DMA((DEPTH_PIECES,)),
                pltpu.SemaphoreType.DMA((heads,)),
                pltpu.SemaphoreType.DMA((6,)),
                pltpu.SemaphoreType.DMA((2 + DEPTH_PIECES,)),
                pltpu.SemaphoreType.DMA((2 + DEPTH_PIECES,)),
                pltpu.SemaphoreType.DMA,
                pltpu.SemaphoreType.DMA,
            ],
            compiler_params=pltpu.CompilerParams(
                collective_id=0, has_side_effects=True, vmem_limit_bytes=60 * 1024 * 1024
            ),
            name="advantages",
        )(hidden.reshape(-1, PACK, width), head_proj, head_out, head_ratio, group_of, lengths, token_mask)

    return jax.shard_map(
        on_device,
        mesh=mesh,
        in_specs=(
            P(("dp", "head"), None, None),
            P("head", None, None),
            P("head", None),
            P(),
            P(),
            P(("dp", "head")),
            P(("dp", "head"), None),
        ),
        out_specs=P(("dp", "head"), None),
        check_vma=False,
    )
```

```python
import functools

import jax
import jax.numpy as jnp
from jax import lax
from jax.experimental import pallas as pl
from jax.experimental.pallas import tpu as pltpu
from jax.sharding import PartitionSpec as P

GROUP = 16
MESH = pl.DeviceIdType.MESH

token_weight = 0.5
gap_weight = 0.5
clip_limit = 2.0
var_offset = 0.04

PACK = 16
LINES = 8
TILE = 256
UNITS = 2
CUT = 6
STEP = 3
AHEAD = 8


def kernel(
    chips,
    hidden, proj, readout, ratio, groups, lens, mask, out,
    rows_all, w_own, w_other, out_own, out_other, comb, ends, msg, slots,
    ratio_s, groups_s, lens_s, groups_v, mask_v,
    pair_recv, all_recv,
):
    chip, core = lax.axis_index("dp"), lax.axis_index("head")
    width = hidden.shape[2]
    count, seq = mask.shape
    heads, _, rank = proj.shape
    devices = 2 * chips
    me = 2 * chip + core
    total_rows = count * seq
    lanes = msg.shape[1]
    tiles = width // TILE
    share = tiles // UNITS
    blocks = total_rows // UNITS // TILE
    pieces = [range(at, min(at + STEP, tiles)) for at in range(0, tiles, STEP)]
    ahead = chip < max(1, chips // AHEAD)

    def columns(span):
        return pl.ds(span[0] * TILE, len(span) * TILE)

    def each_other(act):
        def both(step, _):
            there = lax.rem(chip + step, chips)
            act((there, core))
            act((there, 1 - core))
            return 0

        if chips <= 16:
            for step in range(1, chips):
                both(step, 0)
        else:
            lax.fori_loop(1, chips, both, 0)
        act((chip, 1 - core))

    def reader(values):
        wide = values[...].astype(jnp.float32)
        line = lax.broadcasted_iota(jnp.int32, (PACK, rank), 0)
        parts = [
            jnp.where(line == k, jnp.broadcast_to(wide[k : k + 1], (PACK, rank)), 0.0)
            for k in range(heads)
        ]
        return jnp.concatenate(parts, axis=1).astype(jnp.bfloat16)

    def body(sums, lines, brief, row_sem, w_sem, small_sem, pair_send, all_send):
        first = pltpu.make_async_copy(lens, lens_s, small_sem.at[0])
        small = [
            pltpu.make_async_copy(ratio, ratio_s, small_sem.at[1]),
            pltpu.make_async_copy(groups, groups_s, small_sem.at[2]),
            pltpu.make_async_copy(readout, out_own, small_sem.at[3]),
            pltpu.make_async_copy(groups, groups_v.at[0], small_sem.at[4]),
            pltpu.make_async_copy(mask, mask_v, small_sem.at[5]),
        ]
        w_loads = [
            pltpu.make_async_copy(proj.at[k], w_own.at[:, pl.ds(k * rank, rank)], w_sem.at[k])
            for k in range(heads)
        ]
        h_loads = [
            pltpu.make_async_copy(
                hidden.at[:, :, columns(span)], rows_all.at[:, :, columns(span)], row_sem.at[d]
            )
            for d, span in enumerate([range(CUT), range(CUT, tiles)])
        ]
        for copy in [first] + h_loads:
            copy.start()

        barrier = pltpu.get_barrier_semaphore()
        each_other(
            lambda place: pl.semaphore_signal(
                barrier, inc=1, device_id=place, device_id_type=MESH
            )
        )

        def to_pair(src, dst, k):
            return pltpu.make_async_remote_copy(
                src_ref=src, dst_ref=dst, send_sem=pair_send.at[k], recv_sem=pair_recv.at[k],
                device_id=(chip, 1 - core), device_id_type=MESH,
            )

        send_ends = to_pair(ends.at[0], ends.at[1], 0)
        send_out = to_pair(out_own, out_other, 1)
        send_w = [
            to_pair(w_own.at[columns(span)], w_other.at[columns(span)], 2 + d)
            for d, span in enumerate(pieces)
        ]

        for unit in range(UNITS):
            for ref in sums[unit] + lines[unit] + brief[unit : unit + 1]:
                pltpu.matmul_pop(ref)

        def rows(unit, block, k):
            start = (unit * blocks + block) * (TILE // PACK)
            part = rows_all[pl.ds(start, TILE // PACK), :, pl.ds(k * TILE, TILE)]
            return part.reshape(TILE, TILE)

        def add_tiles(values, span):
            for k in span:
                for unit in range(UNITS):
                    pltpu.matmul_push_rhs(values[pl.ds(k * TILE, TILE), :], k % 2, unit)
                    for block in range(blocks):
                        pltpu.matmul_acc_lhs(
                            sums[unit][block], rows(unit, block, k), None if block else k % 2
                        )

        def add_scores(values, mix, fresh):
            lhs = reader(values)
            for block in range(blocks):
                for unit in range(UNITS):
                    inner = pltpu.matmul_pop(sums[unit][block])
                    active = jnp.tanh(inner).astype(jnp.bfloat16)
                    pltpu.matmul_push_rhs(active, block % 2, unit, transpose=True)
                    pltpu.matmul_acc_lhs(lines[unit][block], lhs, block % 2)
            for block in range(blocks):
                for unit in range(UNITS):
                    per_head = pltpu.matmul_pop(lines[unit][block])
                    line = mix[0] * per_head[0:1]
                    for k in range(1, heads):
                        line = line + mix[k] * per_head[k : k + 1]
                    at = pl.ds((unit * blocks + block) * TILE, TILE)
                    comb[:, at] = line if fresh else comb[:, at] + line

        with jax.named_scope("wait_mid"):
            h_loads[0].wait()
        for copy in w_loads + small:
            copy.start()
        with jax.named_scope("wait_rest"):
            h_loads[1].wait()
            first.wait()

        sub = lax.broadcasted_iota(jnp.int32, (PACK, width), 0)
        picked = jnp.zeros((PACK, width), jnp.float32)
        for r in range(count):
            last = lens_s[r] - 1
            block = rows_all[r * (seq // PACK) + lax.div(last, PACK)].astype(jnp.float32)
            row = jnp.sum(jnp.where(sub == lax.rem(last, PACK), block, 0.0), axis=0, keepdims=True)
            picked = jnp.where(sub == r, jnp.broadcast_to(row, (PACK, width)), picked)
        ends[0] = picked.astype(jnp.bfloat16)[:LINES]

        def mixture(part):
            weights = [ratio_s[k].astype(jnp.float32) for k in range(2 * heads)]
            weight_sum = sum(weights[1:], weights[0])
            return [
                ratio_s[part * heads + k].astype(jnp.float32) / weight_sum for k in range(heads)
            ]

        def own_heads():
            with jax.named_scope("own_tiles"):
                add_tiles(w_own, range(tiles))
            with jax.named_scope("own_scores"):
                add_scores(out_own, mixture(core), True)

        @pl.when(ahead)
        def _():
            for copy in w_loads + small:
                copy.wait()
            own_heads()

        with jax.named_scope("wait_barrier"):
            pl.semaphore_wait(barrier, devices - 1)
        send_ends.start()


        @pl.when(jnp.logical_not(ahead))
        def _():
            with jax.named_scope("wait_w"):
                for copy in w_loads + small:
                    copy.wait()

        send_out.start()

        @pl.when(ahead)
        def _():
            for copy in send_w:
                copy.start()

        own_mix = mixture(core)

        def stage(k):
            for unit in range(UNITS):
                pltpu.matmul_push_rhs(
                    w_own[pl.ds((unit * share + k) * TILE, TILE), :], k % 2, unit
                )

        with jax.named_scope("stage"):
            for k in range(2):
                stage(k)
        with jax.named_scope("wait_ends"):
            send_ends.wait_recv()
        with jax.named_scope("ends_dot"):
            both = ends[...].reshape(2 * LINES, width)
            for k in range(share):
                for unit in range(UNITS):
                    at = (unit * share + k) * TILE
                    pltpu.matmul_acc_lhs(brief[unit], both[:, at : at + TILE], k % 2)
                if k + 2 < share:
                    stage(k + 2)
            inner = pltpu.matmul_pop(brief[0]) + pltpu.matmul_pop(brief[1])
            active = jnp.tanh(inner).astype(jnp.bfloat16).astype(jnp.float32)
            wide = out_own[...].astype(jnp.float32)
            scale = jnp.concatenate([own_mix[k] * wide[k : k + 1] for k in range(heads)], axis=1)
            part = jnp.sum(active * scale, axis=1, keepdims=True)
            line = lax.broadcasted_iota(jnp.int32, (2 * LINES, lanes), 0)
            lane = lax.broadcasted_iota(jnp.int32, (2 * LINES, lanes), 1)
            mine = (line < count) & (lane == me * count + line)
            theirs = (line >= LINES) & (line < LINES + count) & (
                lane == (4 * chip + 1 - me) * count + line - LINES
            )
            note = jnp.sum(jnp.where(mine | theirs, part, 0.0), axis=0, keepdims=True)
            msg[...] = note
            slots[me] = note

        with jax.named_scope("send_all"):
            each_other(
                lambda place: pltpu.make_async_remote_copy(
                    src_ref=msg, dst_ref=slots.at[me], send_sem=all_send.at[0],
                    recv_sem=all_recv, device_id=place, device_id_type=MESH,
                ).start()
            )

        @pl.when(jnp.logical_not(ahead))
        def _():
            for copy in send_w:
                copy.start()
            own_heads()

        send_out.wait_recv()
        for d, span in enumerate(pieces):
            with jax.named_scope(f"wait_other{d}"):
                send_w[d].wait_recv()
            with jax.named_scope(f"other{d}"):
                add_tiles(w_other, span)
        with jax.named_scope("other_scores"):
            add_scores(out_other, mixture(1 - core), False)

        send_ends.wait_send()
        send_out.wait_send()
        for copy in send_w:
            copy.wait_send()
        rest = slots.at[pl.ds(0, devices - 1)]
        pltpu.make_async_copy(rest, rest, all_send.at[0]).wait()

    def acc(unit, size):
        return pltpu.ACC(unit)((size, TILE), jnp.float32)

    pl.run_scoped(
        body,
        [[acc(unit, TILE) for _ in range(blocks)] for unit in range(UNITS)],
        [[acc(unit, PACK) for _ in range(blocks)] for unit in range(UNITS)],
        [acc(unit, 2 * LINES) for unit in range(UNITS)],
        pltpu.SemaphoreType.DMA((2,)),
        pltpu.SemaphoreType.DMA((heads,)),
        pltpu.SemaphoreType.DMA((6,)),
        pltpu.SemaphoreType.DMA((2 + len(pieces),)),
        pltpu.SemaphoreType.DMA((1,)),
    )

    labels = groups_v[...]
    shape = (count, labels.shape[1])
    rollout = lax.broadcasted_iota(jnp.int32, shape, 0)
    lane_of = lax.broadcasted_iota(jnp.int32, shape, 1)
    group = jnp.zeros(shape, jnp.int32)
    length = jnp.zeros((count, seq), jnp.int32)
    line = lax.broadcasted_iota(jnp.int32, (count, seq), 0)
    for r in range(count):
        group = jnp.where(rollout == r, groups_s[me * count + r], group)
        length = jnp.where(line == r, lens_s[r], length)
    member = jnp.broadcast_to(labels, shape) == group
    place = lax.broadcasted_iota(jnp.int32, (count, seq), 1)
    valid = (place < length) & (mask_v[...] == 1)
    tokens = token_weight * jnp.concatenate(
        [comb[:, pl.ds(r * seq, seq)] for r in range(count)], axis=0
    )

    rest = slots.at[pl.ds(0, devices - 1)]
    with jax.named_scope("wait_all"):
        pltpu.make_async_copy(rest, rest, all_recv).wait()

    with jax.named_scope("final"):
        reward = jnp.sum(slots[...], axis=0)[:, : labels.shape[1]]
        wide = jnp.broadcast_to(reward, shape)
        own = jnp.sum(
            jnp.where(lane_of == me * count + rollout, wide, 0.0), axis=1, keepdims=True
        )
        mean = jnp.sum(jnp.where(member, wide, 0.0), axis=1, keepdims=True) / GROUP
        gap = wide - mean
        var = jnp.sum(jnp.where(member, gap * gap, 0.0), axis=1, keepdims=True) / GROUP
        best = jnp.max(jnp.where(member, wide, -jnp.inf), axis=1, keepdims=True)
        base = (own - mean) / jnp.sqrt(var + var_offset) - gap_weight * (best - own)
        shaped = base + tokens
        out[...] = jnp.where(valid, jnp.clip(shaped, -clip_limit, clip_limit), 0.0)


def solution(mesh):
    chips = mesh.shape["dp"]

    def on_device(hidden, head_proj, head_out, head_ratio, group_of, lengths, token_mask):
        count, seq, width = hidden.shape
        heads, _, rank = head_proj.shape
        everyone = group_of.shape[0]
        lanes = -(-everyone // 128) * 128
        pieces = -(-width // (STEP * TILE))
        hbm = pl.BlockSpec(memory_space=pltpu.HBM)
        bf16, f32, i32 = jnp.bfloat16, jnp.float32, jnp.int32
        return pl.pallas_call(
            functools.partial(kernel, chips),
            out_shape=pltpu.VMEM((count, seq), f32),
            in_specs=[hbm] * 7,
            out_specs=pl.BlockSpec(memory_space=pltpu.VMEM),
            scratch_shapes=[
                pltpu.VMEM((count * seq // PACK, PACK, width), bf16),
                pltpu.VMEM((width, heads * rank), bf16),
                pltpu.VMEM((width, heads * rank), bf16),
                pltpu.VMEM((heads, rank), bf16),
                pltpu.VMEM((heads, rank), bf16),
                pltpu.VMEM((1, count * seq), f32),
                pltpu.VMEM((2, LINES, width), bf16),
                pltpu.VMEM((1, lanes), f32),
                pltpu.VMEM((2 * chips, 1, lanes), f32),
                pltpu.SMEM(head_ratio.shape, i32),
                pltpu.SMEM(group_of.shape, i32),
                pltpu.SMEM(lengths.shape, i32),
                pltpu.VMEM((1, everyone), i32),
                pltpu.VMEM((count, seq), i32),
                pltpu.SemaphoreType.DMA((2 + pieces,)),
                pltpu.SemaphoreType.DMA,
            ],
            compiler_params=pltpu.CompilerParams(
                collective_id=0, has_side_effects=True, vmem_limit_bytes=60 * 1024 * 1024
            ),
            name="advantages",
        )(hidden.reshape(-1, PACK, width), head_proj, head_out, head_ratio, group_of, lengths, token_mask)

    return jax.shard_map(
        on_device,
        mesh=mesh,
        in_specs=(
            P(("dp", "head"), None, None),
            P("head", None, None),
            P("head", None),
            P(),
            P(),
            P(("dp", "head")),
            P(("dp", "head"), None),
        ),
        out_specs=P(("dp", "head"), None),
        check_vma=False,
    )
```

```python
import functools

import jax
import jax.numpy as jnp
from jax import lax
from jax.experimental import pallas as pl
from jax.experimental.pallas import tpu as pltpu
from jax.sharding import PartitionSpec as P

GROUP = 16
MESH = pl.DeviceIdType.MESH

token_weight = 0.5
gap_weight = 0.5
clip_limit = 2.0
var_offset = 0.04

PACK = 16
LINES = 8
TILE = 256
UNITS = 2
FAN = 32
AHEAD = 4
FRONT = 8


def mixture(ratio_s, part, heads):
    weights = [ratio_s[k].astype(jnp.float32) for k in range(2 * heads)]
    weight_sum = sum(weights[1:], weights[0])
    return [ratio_s[part * heads + k].astype(jnp.float32) / weight_sum for k in range(heads)]


def gather(
    hidden, proj, readout, ratio, lens, w_front, ends_own, out_own, scale,
    found, lens_s, ratio_s,
):
    core = lax.axis_index("head")
    count = found.shape[0]
    heads, width, rank = proj.shape
    blocks = hidden.shape[0] // count

    def body(sem, w_sem, row_sem):
        first = pltpu.make_async_copy(lens, lens_s, sem.at[0])
        small = [
            pltpu.make_async_copy(ratio, ratio_s, sem.at[1]),
            pltpu.make_async_copy(readout, out_own, sem.at[2]),
        ]
        w_loads = [
            pltpu.make_async_copy(
                proj.at[k, pl.ds(0, FRONT * TILE)], w_front.at[:, pl.ds(k * rank, rank)],
                w_sem.at[k],
            )
            for k in range(heads)
        ]
        for copy in [first] + small + w_loads:
            copy.start()
        with jax.named_scope("gather_lens"):
            first.wait()
        last = [lens_s[r] - 1 for r in range(count)]
        row_loads = [
            pltpu.make_async_copy(
                hidden.at[r * blocks + lax.div(last[r], LINES)], found.at[r], row_sem.at[r]
            )
            for r in range(count)
        ]
        for copy in row_loads:
            copy.start()
        for copy in small:
            copy.wait()
        mix = mixture(ratio_s, core, heads)
        wide = out_own[...].astype(jnp.float32)
        scale[...] = jnp.concatenate([mix[k] * wide[k : k + 1] for k in range(heads)], axis=1)
        with jax.named_scope("gather_rows"):
            for copy in row_loads:
                copy.wait()
        sub = lax.broadcasted_iota(jnp.int32, (LINES, width), 0)
        picked = jnp.zeros((LINES, width), jnp.float32)
        for r in range(count):
            at = sub == lax.rem(last[r], LINES)
            row = jnp.sum(
                jnp.where(at, found[r].astype(jnp.float32), 0.0), axis=0, keepdims=True
            )
            picked = jnp.where(sub == r, jnp.broadcast_to(row, (LINES, width)), picked)
        ends_own[...] = picked.astype(jnp.bfloat16)
        with jax.named_scope("gather_w"):
            for copy in w_loads:
                copy.wait()

    pl.run_scoped(
        body,
        pltpu.SemaphoreType.DMA((3,)),
        pltpu.SemaphoreType.DMA((heads,)),
        pltpu.SemaphoreType.DMA((count,)),
    )


def kernel(
    chips,
    hidden, proj, w_front, ends_own, out_own, scale, ratio, groups, lens, mask, out,
    rows_all, w_back, w_other, out_other, comb, ends, msg, slots,
    ratio_s, groups_s, lens_s, groups_v, mask_v,
    pair_recv, all_recv, here,
):
    chip, core = lax.axis_index("dp"), lax.axis_index("head")
    width = hidden.shape[2]
    count, seq = mask.shape
    heads, rank = out_own.shape
    devices = 2 * chips
    me = 2 * chip + core
    total_rows = count * seq
    lanes = msg.shape[1]
    tiles = width // TILE
    spans = [range(FRONT), range(FRONT, tiles)]
    blocks = total_rows // UNITS // TILE
    pieces = [range(FRONT), range(FRONT, tiles)]
    ahead = chip < max(1, chips // AHEAD)

    def columns(span):
        return pl.ds(span[0] * TILE, len(span) * TILE)

    def cores(act, low, high):
        def both(there, _):
            act((there, core))
            act((there, 1 - core))
            return 0

        lax.fori_loop(low, high, both, 0)

    def reader(values):
        wide = values[...].astype(jnp.float32)
        line = lax.broadcasted_iota(jnp.int32, (PACK, rank), 0)
        parts = [
            jnp.where(line == k, jnp.broadcast_to(wide[k : k + 1], (PACK, rank)), 0.0)
            for k in range(heads)
        ]
        return jnp.concatenate(parts, axis=1).astype(jnp.bfloat16)

    def body(sums, lines, brief, row_sem, w_sem, small_sem, pair_send, all_send):
        small = [
            pltpu.make_async_copy(ratio, ratio_s, small_sem.at[0]),
            pltpu.make_async_copy(lens, lens_s, small_sem.at[1]),
            pltpu.make_async_copy(groups, groups_s, small_sem.at[2]),
            pltpu.make_async_copy(groups, groups_v.at[0], small_sem.at[3]),
            pltpu.make_async_copy(mask, mask_v, small_sem.at[4]),
        ]
        h_loads = [
            pltpu.make_async_copy(
                hidden.at[:, :, columns(span)], rows_all.at[:, :, columns(span)], row_sem.at[d]
            )
            for d, span in enumerate(spans)
        ]
        w_loads = [
            pltpu.make_async_copy(
                proj.at[k, columns(range(FRONT, tiles))], w_back.at[:, pl.ds(k * rank, rank)],
                w_sem.at[k],
            )
            for k in range(heads)
        ]
        for copy in w_loads:
            copy.start()

        barrier = pltpu.get_barrier_semaphore()

        def hello(place):
            pl.semaphore_signal(barrier, inc=1, device_id=place, device_id_type=MESH)

        hello((chip, 1 - core))
        for copy in h_loads + small:
            copy.start()
        cores(hello, chip + 1, chips)
        ends[0] = ends_own[...]

        def to_pair(src, dst, k):
            return pltpu.make_async_remote_copy(
                src_ref=src, dst_ref=dst, send_sem=pair_send.at[k], recv_sem=pair_recv.at[k],
                device_id=(chip, 1 - core), device_id_type=MESH,
            )

        send_ends = to_pair(ends_own, ends.at[1], 0)
        send_out = to_pair(out_own, out_other, 1)
        def own_piece(span):
            return w_front if span[0] < FRONT else w_back

        send_w = [
            to_pair(own_piece(span), w_other.at[columns(span)], 2 + d)
            for d, span in enumerate(pieces)
        ]

        for unit in range(UNITS):
            for ref in sums[unit] + lines[unit] + brief[unit : unit + 1]:
                pltpu.matmul_pop(ref)

        def own_tile(k):
            ref, at = (w_front, k) if k < FRONT else (w_back, k - FRONT)
            return ref[pl.ds(at * TILE, TILE), :]

        def other_tile(k):
            return w_other[pl.ds(k * TILE, TILE), :]

        def rows(unit, block, k):
            start = (unit * blocks + block) * (TILE // PACK)
            part = rows_all[pl.ds(start, TILE // PACK), :, pl.ds(k * TILE, TILE)]
            return part.reshape(TILE, TILE)

        def add_tiles(tile, span):
            for k in span:
                for unit in range(UNITS):
                    pltpu.matmul_push_rhs(tile(k), k % 2, unit)
                    for block in range(blocks):
                        pltpu.matmul_acc_lhs(
                            sums[unit][block], rows(unit, block, k), None if block else k % 2
                        )

        def add_scores(values, mix, fresh):
            lhs = reader(values)
            for block in range(blocks):
                for unit in range(UNITS):
                    inner = pltpu.matmul_pop(sums[unit][block])
                    active = jnp.tanh(inner).astype(jnp.bfloat16)
                    pltpu.matmul_push_rhs(active, block % 2, unit, transpose=True)
                    pltpu.matmul_acc_lhs(lines[unit][block], lhs, block % 2)
            for block in range(blocks):
                for unit in range(UNITS):
                    per_head = pltpu.matmul_pop(lines[unit][block])
                    line = mix[0] * per_head[0:1]
                    for k in range(1, heads):
                        line = line + mix[k] * per_head[k : k + 1]
                    at = pl.ds((unit * blocks + block) * TILE, TILE)
                    comb[:, at] = line if fresh else comb[:, at] + line

        def own_heads():
            for d, span in enumerate(spans):
                with jax.named_scope(f"wait_hidden{d}"):
                    h_loads[d].wait()
                with jax.named_scope(f"own_tiles{d}"):
                    add_tiles(own_tile, span)
            with jax.named_scope("own_scores"):
                small[0].wait()
                add_scores(out_own, mixture(ratio_s, core, heads), True)

        with jax.named_scope("wait_barrier"):
            pl.semaphore_wait(barrier, 2 * chip + 1)
        send_ends.start()
        send_out.start()

        @pl.when(ahead)
        def _():
            send_w[0].start()

        cores(
            lambda place: pl.semaphore_signal(
                here, inc=1, device_id=place, device_id_type=MESH
            ),
            0, chip,
        )

        turns = [range(at, at + UNITS) for at in range(0, tiles, UNITS)]

        def stage(turn):
            for unit, k in enumerate(turns[turn]):
                pltpu.matmul_push_rhs(own_tile(k), turn % 2, unit)

        for turn in range(2):
            stage(turn)
        with jax.named_scope("wait_w"):
            for copy in w_loads:
                copy.wait()

        @pl.when(ahead)
        def _():
            send_w[1].start()

        with jax.named_scope("wait_ends"):
            send_ends.wait_recv()
        with jax.named_scope("ends_dot"):
            both = ends[...].reshape(2 * LINES, width)
            for turn, units in enumerate(turns):
                for unit, k in enumerate(units):
                    at = k * TILE
                    pltpu.matmul_acc_lhs(brief[unit], both[:, at : at + TILE], turn % 2)
                if turn + 2 < len(turns):
                    stage(turn + 2)
            inner = pltpu.matmul_pop(brief[0]) + pltpu.matmul_pop(brief[1])
            active = jnp.tanh(inner).astype(jnp.bfloat16).astype(jnp.float32)
            part = jnp.sum(active * scale[...], axis=1, keepdims=True)
            line = lax.broadcasted_iota(jnp.int32, (2 * LINES, lanes), 0)
            lane = lax.broadcasted_iota(jnp.int32, (2 * LINES, lanes), 1)
            mine = (line < count) & (lane == me * count + line)
            theirs = (line >= LINES) & (line < LINES + count) & (
                lane == (4 * chip + 1 - me) * count + line - LINES
            )
            found = jnp.where(mine | theirs, part, 0.0)
            found = found[:LINES] + found[LINES:]
            note = sum([found[r : r + 1] for r in range(1, count)], found[:1])
            msg[...] = note
            slots[me] = note

        def tell(place):
            pltpu.make_async_remote_copy(
                src_ref=msg, dst_ref=slots.at[me], send_sem=all_send.at[0],
                recv_sem=all_recv, device_id=place, device_id_type=MESH,
            ).start()

        with jax.named_scope("send_lower"):
            cores(tell, 0, chip)
            tell((chip, 1 - core))

        @pl.when(ahead)
        def _():
            own_heads()

        @pl.when(chip < chips - 1)
        def _():
            with jax.named_scope("wait_higher"):
                pl.semaphore_wait(here, devices - 2 - 2 * chip)

        with jax.named_scope("send_higher"):
            cores(tell, chip + 1, chips)

        @pl.when(jnp.logical_not(ahead))
        def _():
            for copy in send_w:
                copy.start()
            own_heads()

        send_out.wait_recv()
        for d, span in enumerate(pieces):
            with jax.named_scope(f"wait_other{d}"):
                send_w[d].wait_recv()
            with jax.named_scope(f"other{d}"):
                add_tiles(other_tile, span)
        with jax.named_scope("other_scores"):
            add_scores(out_other, mixture(ratio_s, 1 - core, heads), False)

        for copy in small[1:]:
            copy.wait()
        send_ends.wait_send()
        send_out.wait_send()
        for copy in send_w:
            copy.wait_send()
        rest = slots.at[pl.ds(0, devices - 1)]
        pltpu.make_async_copy(rest, rest, all_send.at[0]).wait()

    def acc(unit, size):
        return pltpu.ACC(unit)((size, TILE), jnp.float32)

    pl.run_scoped(
        body,
        [[acc(unit, TILE) for _ in range(blocks)] for unit in range(UNITS)],
        [[acc(unit, PACK) for _ in range(blocks)] for unit in range(UNITS)],
        [acc(unit, 2 * LINES) for unit in range(UNITS)],
        pltpu.SemaphoreType.DMA((2,)),
        pltpu.SemaphoreType.DMA((heads,)),
        pltpu.SemaphoreType.DMA((5,)),
        pltpu.SemaphoreType.DMA((2 + len(pieces),)),
        pltpu.SemaphoreType.DMA((1,)),
    )

    labels = groups_v[...]
    shape = (count, labels.shape[1])
    rollout = lax.broadcasted_iota(jnp.int32, shape, 0)
    lane_of = lax.broadcasted_iota(jnp.int32, shape, 1)
    group = jnp.zeros(shape, jnp.int32)
    length = jnp.zeros((count, seq), jnp.int32)
    line = lax.broadcasted_iota(jnp.int32, (count, seq), 0)
    for r in range(count):
        group = jnp.where(rollout == r, groups_s[me * count + r], group)
        length = jnp.where(line == r, lens_s[r], length)
    member = jnp.broadcast_to(labels, shape) == group
    place = lax.broadcasted_iota(jnp.int32, (count, seq), 1)
    valid = (place < length) & (mask_v[...] == 1)
    tokens = token_weight * jnp.concatenate(
        [comb[:, pl.ds(r * seq, seq)] for r in range(count)], axis=0
    )

    rest = slots.at[pl.ds(0, devices - 1)]
    with jax.named_scope("wait_all"):
        pltpu.make_async_copy(rest, rest, all_recv).wait()

    with jax.named_scope("final"):
        level = [slots[k] for k in range(min(devices, FAN))]
        for k in range(FAN, devices):
            level[k % FAN] = level[k % FAN] + slots[k]
        while len(level) > 1:
            level = [sum(level[k + 1 : k + 2], level[k]) for k in range(0, len(level), 2)]
        reward = level[0][:, : labels.shape[1]]
        wide = jnp.broadcast_to(reward, shape)
        own = jnp.sum(
            jnp.where(lane_of == me * count + rollout, wide, 0.0), axis=1, keepdims=True
        )
        mean = jnp.sum(jnp.where(member, wide, 0.0), axis=1, keepdims=True) * (1 / GROUP)
        gap = wide - mean
        var = jnp.sum(jnp.where(member, gap * gap, 0.0), axis=1, keepdims=True) * (1 / GROUP)
        best = jnp.max(jnp.where(member, wide, -jnp.inf), axis=1, keepdims=True)
        base = (own - mean) * lax.rsqrt(var + var_offset) - gap_weight * (best - own)
        shaped = base + tokens
        out[...] = jnp.where(valid, jnp.clip(shaped, -clip_limit, clip_limit), 0.0)


def solution(mesh):
    chips = mesh.shape["dp"]

    def on_device(hidden, head_proj, head_out, head_ratio, group_of, lengths, token_mask):
        count, seq, width = hidden.shape
        heads, _, rank = head_proj.shape
        everyone = group_of.shape[0]
        lanes = -(-everyone // 128) * 128
        pieces = 2
        hbm = pl.BlockSpec(memory_space=pltpu.HBM)
        bf16, f32, i32 = jnp.bfloat16, jnp.float32, jnp.int32
        vmem = pl.BlockSpec(memory_space=pltpu.VMEM)
        rows = hidden.reshape(-1, PACK, width)
        early = pl.pallas_call(
            gather,
            out_shape=[
                pltpu.VMEM((FRONT * TILE, heads * rank), bf16),
                pltpu.VMEM((LINES, width), bf16),
                pltpu.VMEM((heads, rank), bf16),
                pltpu.VMEM((1, heads * rank), f32),
            ],
            in_specs=[hbm] * 5,
            out_specs=[vmem] * 4,
            scratch_shapes=[
                pltpu.VMEM((count, LINES, width), bf16),
                pltpu.SMEM(lengths.shape, i32),
                pltpu.SMEM(head_ratio.shape, i32),
            ],
            compiler_params=pltpu.CompilerParams(vmem_limit_bytes=60 * 1024 * 1024),
            name="gather",
        )(hidden.reshape(-1, LINES, width), head_proj, head_out, head_ratio, lengths)
        early = [pltpu.with_memory_space_constraint(value, pltpu.VMEM) for value in early]
        return pl.pallas_call(
            functools.partial(kernel, chips),
            out_shape=pltpu.VMEM((count, seq), f32),
            in_specs=[hbm] * 2 + [vmem] * 4 + [hbm] * 4,
            out_specs=pl.BlockSpec(memory_space=pltpu.VMEM),
            scratch_shapes=[
                pltpu.VMEM((count * seq // PACK, PACK, width), bf16),
                pltpu.VMEM((width - FRONT * TILE, heads * rank), bf16),
                pltpu.VMEM((width, heads * rank), bf16),
                pltpu.VMEM((heads, rank), bf16),
                pltpu.VMEM((1, count * seq), f32),
                pltpu.VMEM((2, LINES, width), bf16),
                pltpu.VMEM((1, lanes), f32),
                pltpu.VMEM((2 * chips, 1, lanes), f32),
                pltpu.SMEM(head_ratio.shape, i32),
                pltpu.SMEM(group_of.shape, i32),
                pltpu.SMEM(lengths.shape, i32),
                pltpu.VMEM((1, everyone), i32),
                pltpu.VMEM((count, seq), i32),
                pltpu.SemaphoreType.DMA((2 + pieces,)),
                pltpu.SemaphoreType.DMA,
                pltpu.SemaphoreType.REGULAR,
            ],
            compiler_params=pltpu.CompilerParams(
                collective_id=0, has_side_effects=True, vmem_limit_bytes=60 * 1024 * 1024
            ),
            name="advantages",
        )(rows, head_proj, *early, head_ratio, group_of, lengths, token_mask)

    return jax.shard_map(
        on_device,
        mesh=mesh,
        in_specs=(
            P(("dp", "head"), None, None),
            P("head", None, None),
            P("head", None),
            P(),
            P(),
            P(("dp", "head")),
            P(("dp", "head"), None),
        ),
        out_specs=P(("dp", "head"), None),
        check_vma=False,
    )
```

```python
import functools

import jax
import jax.numpy as jnp
from jax import lax
from jax.experimental import pallas as pl
from jax.experimental.pallas import tpu as pltpu
from jax.sharding import PartitionSpec as P

GROUP = 16
MESH = pl.DeviceIdType.MESH

token_weight = 0.5
gap_weight = 0.5
clip_limit = 2.0
var_offset = 0.04

PACK = 16
LINES = 8
TILE = 256
UNITS = 2
FAN = 32
AHEAD = 2
FRONT = 8


def mixture(ratio_s, part, heads):
    weights = [ratio_s[k].astype(jnp.float32) for k in range(2 * heads)]
    weight_sum = sum(weights[1:], weights[0])
    return [ratio_s[part * heads + k].astype(jnp.float32) / weight_sum for k in range(heads)]


def gather(
    hidden, proj, readout, ratio, lens, w_front, ends_own, out_own, scale,
    found, lens_s, ratio_s,
):
    core = lax.axis_index("head")
    count = found.shape[0]
    heads, width, rank = proj.shape
    blocks = hidden.shape[0] // count

    def body(sem, w_sem, row_sem):
        first = pltpu.make_async_copy(lens, lens_s, sem.at[0])
        small = [
            pltpu.make_async_copy(ratio, ratio_s, sem.at[1]),
            pltpu.make_async_copy(readout, out_own, sem.at[2]),
        ]
        w_loads = [
            pltpu.make_async_copy(
                proj.at[k, pl.ds(0, FRONT * TILE)], w_front.at[:, pl.ds(k * rank, rank)],
                w_sem.at[k],
            )
            for k in range(heads)
        ]
        for copy in [first] + small + w_loads:
            copy.start()
        with jax.named_scope("gather_lens"):
            first.wait()
        last = [lens_s[r] - 1 for r in range(count)]
        row_loads = [
            pltpu.make_async_copy(
                hidden.at[r * blocks + lax.div(last[r], LINES)], found.at[r], row_sem.at[r]
            )
            for r in range(count)
        ]
        for copy in row_loads:
            copy.start()
        for copy in small:
            copy.wait()
        mix = mixture(ratio_s, core, heads)
        wide = out_own[...].astype(jnp.float32)
        scale[...] = jnp.concatenate([mix[k] * wide[k : k + 1] for k in range(heads)], axis=1)
        with jax.named_scope("gather_rows"):
            for copy in row_loads:
                copy.wait()
        sub = lax.broadcasted_iota(jnp.int32, (LINES, width), 0)
        picked = jnp.zeros((LINES, width), jnp.float32)
        for r in range(count):
            block = found[r].astype(jnp.float32)
            turned = pltpu.roll(block, lax.rem(LINES + r - lax.rem(last[r], LINES), LINES), 0)
            picked = jnp.where(sub == r, turned, picked)
        lead = picked[:, :rank]
        for k in range(heads):
            at = sub[:, :rank] == count + k
            lead = jnp.where(at, jnp.broadcast_to(wide[k : k + 1], (LINES, rank)), lead)
        picked = jnp.concatenate([lead, picked[:, rank:]], axis=1)
        ends_own[...] = picked[: count + heads].astype(jnp.bfloat16)
        with jax.named_scope("gather_w"):
            for copy in w_loads:
                copy.wait()

    pl.run_scoped(
        body,
        pltpu.SemaphoreType.DMA((3,)),
        pltpu.SemaphoreType.DMA((heads,)),
        pltpu.SemaphoreType.DMA((count,)),
    )


def kernel(
    chips,
    hidden, proj, w_front, ends_own, out_own, scale, ratio, groups, lens, mask, out,
    rows_all, w_back, w_other, comb, ends, msg, slots,
    ratio_s, groups_s, lens_s, groups_v, mask_v,
    pair_recv, all_recv, here,
):
    chip, core = lax.axis_index("dp"), lax.axis_index("head")
    width = hidden.shape[2]
    count, seq = mask.shape
    heads, rank = out_own.shape
    devices = 2 * chips
    me = 2 * chip + core
    total_rows = count * seq
    lanes = msg.shape[1]
    tiles = width // TILE
    spans = [range(FRONT), range(FRONT, tiles)]
    blocks = total_rows // UNITS // TILE
    pieces = [range(FRONT), range(FRONT, tiles)]
    ahead = chip < max(1, chips // AHEAD)

    def columns(span):
        return pl.ds(span[0] * TILE, len(span) * TILE)

    def cores(act, low, high):
        def both(there, _):
            act((there, core))
            act((there, 1 - core))
            return 0

        lax.fori_loop(low, high, both, 0)

    def reader(values):
        wide = values.astype(jnp.float32)
        line = lax.broadcasted_iota(jnp.int32, (PACK, rank), 0)
        parts = [
            jnp.where(line == k, jnp.broadcast_to(wide[k : k + 1], (PACK, rank)), 0.0)
            for k in range(heads)
        ]
        return jnp.concatenate(parts, axis=1).astype(jnp.bfloat16)

    def body(sums, lines, brief, row_sem, w_sem, small_sem, pair_send, all_send):
        small = [
            pltpu.make_async_copy(ratio, ratio_s, small_sem.at[0]),
            pltpu.make_async_copy(lens, lens_s, small_sem.at[1]),
            pltpu.make_async_copy(groups, groups_s, small_sem.at[2]),
            pltpu.make_async_copy(groups, groups_v.at[0], small_sem.at[3]),
            pltpu.make_async_copy(mask, mask_v, small_sem.at[4]),
        ]
        h_loads = [
            pltpu.make_async_copy(
                hidden.at[:, :, columns(span)], rows_all.at[:, :, columns(span)], row_sem.at[d]
            )
            for d, span in enumerate(spans)
        ]
        w_loads = [
            pltpu.make_async_copy(
                proj.at[k, columns(range(FRONT, tiles))], w_back.at[:, pl.ds(k * rank, rank)],
                w_sem.at[k],
            )
            for k in range(heads)
        ]

        barrier = pltpu.get_barrier_semaphore()

        def hello(place):
            pl.semaphore_signal(barrier, inc=1, device_id=place, device_id_type=MESH)

        hello((chip, 1 - core))
        for copy in w_loads:
            copy.start()
        cores(hello, chip + 1, chips)
        for copy in h_loads + small:
            copy.start()

        def to_pair(src, dst, k):
            return pltpu.make_async_remote_copy(
                src_ref=src, dst_ref=dst, send_sem=pair_send.at[k], recv_sem=pair_recv.at[k],
                device_id=(chip, 1 - core), device_id_type=MESH,
            )

        send_ends = to_pair(ends_own, ends, 0)
        def own_piece(span):
            return w_front if span[0] < FRONT else w_back

        send_w = [
            pltpu.make_async_remote_copy(
                src_ref=own_piece(span), dst_ref=w_other.at[columns(span)],
                send_sem=pair_send.at[1 + d], recv_sem=pair_recv.at[1 + d],
                device_id=(chip, 1 - core), device_id_type=MESH,
            )
            for d, span in enumerate(pieces)
        ]

        for unit in range(UNITS):
            for ref in sums[unit] + lines[unit] + brief[unit : unit + 1]:
                pltpu.matmul_pop(ref)

        def own_tile(k):
            ref, at = (w_front, k) if k < FRONT else (w_back, k - FRONT)
            return ref[pl.ds(at * TILE, TILE), :]

        def other_tile(k):
            return w_other[pl.ds(k * TILE, TILE), :]

        def rows(unit, block, k):
            start = (unit * blocks + block) * (TILE // PACK)
            part = rows_all[pl.ds(start, TILE // PACK), :, pl.ds(k * TILE, TILE)]
            return part.reshape(TILE, TILE)

        def add_tiles(tile, span):
            for k in span:
                for unit in range(UNITS):
                    pltpu.matmul_push_rhs(tile(k), k % 2, unit)
                    for block in range(blocks):
                        pltpu.matmul_acc_lhs(
                            sums[unit][block], rows(unit, block, k), None if block else k % 2
                        )

        def add_scores(values, mix, fresh):
            lhs = reader(values)
            for block in range(blocks):
                for unit in range(UNITS):
                    inner = pltpu.matmul_pop(sums[unit][block])
                    active = jnp.tanh(inner).astype(jnp.bfloat16)
                    pltpu.matmul_push_rhs(active, block % 2, unit, transpose=True)
                    pltpu.matmul_acc_lhs(lines[unit][block], lhs, block % 2)
            for block in range(blocks):
                for unit in range(UNITS):
                    per_head = pltpu.matmul_pop(lines[unit][block])
                    line = mix[0] * per_head[0:1]
                    for k in range(1, heads):
                        line = line + mix[k] * per_head[k : k + 1]
                    at = pl.ds((unit * blocks + block) * TILE, TILE)
                    comb[:, at] = line if fresh else comb[:, at] + line

        def own_heads():
            for d, span in enumerate(spans):
                with jax.named_scope(f"wait_hidden{d}"):
                    h_loads[d].wait()
                with jax.named_scope(f"own_tiles{d}"):
                    add_tiles(own_tile, span)
            with jax.named_scope("own_scores"):
                small[0].wait()
                add_scores(out_own[...], mixture(ratio_s, core, heads), True)

        with jax.named_scope("wait_barrier"):
            pl.semaphore_wait(barrier, 2 * chip + 1)
        send_ends.start()

        @pl.when(ahead)
        def _():
            send_w[0].start()

        cores(
            lambda place: pl.semaphore_signal(
                here, inc=1, device_id=place, device_id_type=MESH
            ),
            0, chip,
        )

        turns = [range(at, at + UNITS) for at in range(0, tiles, UNITS)]

        def stage(turn):
            for unit, k in enumerate(turns[turn]):
                pltpu.matmul_push_rhs(own_tile(k), turn % 2, unit)

        lot = count + heads

        def lines_of(k, own, other):
            at = pl.ds(k * TILE, TILE)
            blank = jnp.zeros((lot, TILE), jnp.float32)
            stack = [
                ends_own[:, at].astype(jnp.float32) if own else blank,
                ends[:, at].astype(jnp.float32) if other else blank,
                jnp.zeros((PACK - 2 * lot, TILE), jnp.float32),
            ]
            return jnp.concatenate(stack, axis=0).astype(jnp.bfloat16)

        def add_lines(turn, own, other, load):
            for unit, k in enumerate(turns[turn]):
                pltpu.matmul_acc_lhs(brief[unit], lines_of(k, own, other), load)

        stage(0)
        stage(1)
        add_lines(0, True, False, 0)
        stage(2)
        with jax.named_scope("wait_w"):
            for copy in w_loads:
                copy.wait()

        @pl.when(ahead)
        def _():
            send_w[1].start()

        with jax.named_scope("wait_ends"):
            send_ends.wait_recv()
        with jax.named_scope("ends_dot"):
            add_lines(0, False, True, None)
            for turn in range(1, len(turns)):
                add_lines(turn, True, True, turn % 2)
                if turn + 2 < len(turns):
                    stage(turn + 2)
            inner = pltpu.matmul_pop(brief[0]) + pltpu.matmul_pop(brief[1])
            inner = inner[:LINES]
            active = jnp.tanh(inner).astype(jnp.bfloat16).astype(jnp.float32)
            part = jnp.sum(active * scale[...], axis=1, keepdims=True)
            line = lax.broadcasted_iota(jnp.int32, (LINES, lanes), 0)
            lane = lax.broadcasted_iota(jnp.int32, (LINES, lanes), 1)
            mine = (line < count) & (lane == me * count + line)
            theirs = (line >= lot) & (line < lot + count) & (
                lane == (4 * chip + 1 - me) * count + line - lot
            )
            found = jnp.where(mine | theirs, part, 0.0)
            found = found + pltpu.roll(found, lot, 0)
            note = sum([found[r : r + 1] for r in range(1, count)], found[:1])
            msg[...] = note
            slots[me] = note

        def tell(place):
            pltpu.make_async_remote_copy(
                src_ref=msg, dst_ref=slots.at[me], send_sem=all_send.at[0],
                recv_sem=all_recv, device_id=place, device_id_type=MESH,
            ).start()

        with jax.named_scope("send_lower"):
            cores(tell, 0, chip)
            tell((chip, 1 - core))

        @pl.when(ahead)
        def _():
            own_heads()

        @pl.when(chip < chips - 1)
        def _():
            with jax.named_scope("wait_higher"):
                pl.semaphore_wait(here, devices - 2 - 2 * chip)

        with jax.named_scope("send_higher"):
            cores(tell, chip + 1, chips)

        @pl.when(jnp.logical_not(ahead))
        def _():
            for copy in send_w:
                copy.start()
            own_heads()

        for d, span in enumerate(pieces):
            with jax.named_scope(f"wait_other{d}"):
                send_w[d].wait_recv()
            with jax.named_scope(f"other{d}"):
                add_tiles(other_tile, span)
        with jax.named_scope("other_scores"):
            values = ends[:, :rank].astype(jnp.float32)[count:]
            add_scores(values, mixture(ratio_s, 1 - core, heads), False)

        for copy in small[1:]:
            copy.wait()
        send_ends.wait_send()
        for copy in send_w:
            copy.wait_send()
        rest = slots.at[pl.ds(0, devices - 1)]
        pltpu.make_async_copy(rest, rest, all_send.at[0]).wait()

    def acc(unit, size):
        return pltpu.ACC(unit)((size, TILE), jnp.float32)

    pl.run_scoped(
        body,
        [[acc(unit, TILE) for _ in range(blocks)] for unit in range(UNITS)],
        [[acc(unit, PACK) for _ in range(blocks)] for unit in range(UNITS)],
        [acc(unit, PACK) for unit in range(UNITS)],
        pltpu.SemaphoreType.DMA((2,)),
        pltpu.SemaphoreType.DMA((heads,)),
        pltpu.SemaphoreType.DMA((5,)),
        pltpu.SemaphoreType.DMA((1 + len(pieces),)),
        pltpu.SemaphoreType.DMA((1,)),
    )

    labels = groups_v[...]
    shape = (count, labels.shape[1])
    rollout = lax.broadcasted_iota(jnp.int32, shape, 0)
    lane_of = lax.broadcasted_iota(jnp.int32, shape, 1)
    group = jnp.zeros(shape, jnp.int32)
    length = jnp.zeros((count, seq), jnp.int32)
    line = lax.broadcasted_iota(jnp.int32, (count, seq), 0)
    for r in range(count):
        group = jnp.where(rollout == r, groups_s[me * count + r], group)
        length = jnp.where(line == r, lens_s[r], length)
    member = jnp.broadcast_to(labels, shape) == group
    place = lax.broadcasted_iota(jnp.int32, (count, seq), 1)
    valid = (place < length) & (mask_v[...] == 1)
    tokens = token_weight * jnp.concatenate(
        [comb[:, pl.ds(r * seq, seq)] for r in range(count)], axis=0
    )

    rest = slots.at[pl.ds(0, devices - 1)]
    with jax.named_scope("wait_all"):
        pltpu.make_async_copy(rest, rest, all_recv).wait()

    with jax.named_scope("final"):
        level = [slots[k] for k in range(min(devices, FAN))]
        for k in range(FAN, devices):
            level[k % FAN] = level[k % FAN] + slots[k]
        while len(level) > 1:
            level = [sum(level[k + 1 : k + 2], level[k]) for k in range(0, len(level), 2)]
        reward = level[0][:, : labels.shape[1]]
        wide = jnp.broadcast_to(reward, shape)
        own = jnp.sum(
            jnp.where(lane_of == me * count + rollout, wide, 0.0), axis=1, keepdims=True
        )
        mean = jnp.sum(jnp.where(member, wide, 0.0), axis=1, keepdims=True) * (1 / GROUP)
        gap = wide - mean
        var = jnp.sum(jnp.where(member, gap * gap, 0.0), axis=1, keepdims=True) * (1 / GROUP)
        best = jnp.max(jnp.where(member, wide, -jnp.inf), axis=1, keepdims=True)
        base = (own - mean) * lax.rsqrt(var + var_offset) - gap_weight * (best - own)
        shaped = base + tokens
        out[...] = jnp.where(valid, jnp.clip(shaped, -clip_limit, clip_limit), 0.0)


def solution(mesh):
    chips = mesh.shape["dp"]

    def on_device(hidden, head_proj, head_out, head_ratio, group_of, lengths, token_mask):
        count, seq, width = hidden.shape
        heads, _, rank = head_proj.shape
        everyone = group_of.shape[0]
        lanes = -(-everyone // 128) * 128
        pieces = 2
        hbm = pl.BlockSpec(memory_space=pltpu.HBM)
        bf16, f32, i32 = jnp.bfloat16, jnp.float32, jnp.int32
        vmem = pl.BlockSpec(memory_space=pltpu.VMEM)
        rows = hidden.reshape(-1, PACK, width)
        early = pl.pallas_call(
            gather,
            out_shape=[
                pltpu.VMEM((FRONT * TILE, heads * rank), bf16),
                pltpu.VMEM((count + heads, width), bf16),
                pltpu.VMEM((heads, rank), bf16),
                pltpu.VMEM((1, heads * rank), f32),
            ],
            in_specs=[hbm] * 5,
            out_specs=[vmem] * 4,
            scratch_shapes=[
                pltpu.VMEM((count, LINES, width), bf16),
                pltpu.SMEM(lengths.shape, i32),
                pltpu.SMEM(head_ratio.shape, i32),
            ],
            compiler_params=pltpu.CompilerParams(vmem_limit_bytes=60 * 1024 * 1024),
            name="gather",
        )(hidden.reshape(-1, LINES, width), head_proj, head_out, head_ratio, lengths)
        early = [pltpu.with_memory_space_constraint(value, pltpu.VMEM) for value in early]
        return pl.pallas_call(
            functools.partial(kernel, chips),
            out_shape=pltpu.VMEM((count, seq), f32),
            in_specs=[hbm] * 2 + [vmem] * 4 + [hbm] * 4,
            out_specs=pl.BlockSpec(memory_space=pltpu.VMEM),
            scratch_shapes=[
                pltpu.VMEM((count * seq // PACK, PACK, width), bf16),
                pltpu.VMEM((width - FRONT * TILE, heads * rank), bf16),
                pltpu.VMEM((width, heads * rank), bf16),
                pltpu.VMEM((1, count * seq), f32),
                pltpu.VMEM((count + heads, width), bf16),
                pltpu.VMEM((1, lanes), f32),
                pltpu.VMEM((2 * chips, 1, lanes), f32),
                pltpu.SMEM(head_ratio.shape, i32),
                pltpu.SMEM(group_of.shape, i32),
                pltpu.SMEM(lengths.shape, i32),
                pltpu.VMEM((1, everyone), i32),
                pltpu.VMEM((count, seq), i32),
                pltpu.SemaphoreType.DMA((1 + pieces,)),
                pltpu.SemaphoreType.DMA,
                pltpu.SemaphoreType.REGULAR,
            ],
            compiler_params=pltpu.CompilerParams(
                collective_id=0, has_side_effects=True, vmem_limit_bytes=60 * 1024 * 1024
            ),
            name="advantages",
        )(rows, head_proj, *early, head_ratio, group_of, lengths, token_mask)

    return jax.shard_map(
        on_device,
        mesh=mesh,
        in_specs=(
            P(("dp", "head"), None, None),
            P("head", None, None),
            P("head", None),
            P(),
            P(),
            P(("dp", "head")),
            P(("dp", "head"), None),
        ),
        out_specs=P(("dp", "head"), None),
        check_vma=False,
    )
```

```python
import functools

import jax
import jax.numpy as jnp
from jax import lax
from jax.experimental import pallas as pl
from jax.experimental.pallas import tpu as pltpu
from jax.sharding import PartitionSpec as P

GROUP = 16
MESH = pl.DeviceIdType.MESH

token_weight = 0.5
gap_weight = 0.5
clip_limit = 2.0
var_offset = 0.04

PACK = 16
LINES = 8
TILE = 256
UNITS = 2
AHEAD = 2
LEAD = 16
WAVES = 2
FRONT = 8


def mixture(ratio_s, part, heads):
    weights = [ratio_s[k].astype(jnp.float32) for k in range(2 * heads)]
    weight_sum = sum(weights[1:], weights[0])
    return [ratio_s[part * heads + k].astype(jnp.float32) / weight_sum for k in range(heads)]


def gather(
    hidden, proj, readout, ratio, lens, w_front, ends_own, out_own, scale,
    found, lens_s, ratio_s,
):
    core = lax.axis_index("head")
    count = found.shape[0]
    heads, width, rank = proj.shape
    blocks = hidden.shape[0] // count

    def body(sem, w_sem, row_sem):
        first = pltpu.make_async_copy(lens, lens_s, sem.at[0])
        small = [
            pltpu.make_async_copy(ratio, ratio_s, sem.at[1]),
            pltpu.make_async_copy(readout, out_own, sem.at[2]),
        ]
        w_loads = [
            pltpu.make_async_copy(
                proj.at[k, pl.ds(0, FRONT * TILE)], w_front.at[:, pl.ds(k * rank, rank)],
                w_sem.at[k],
            )
            for k in range(heads)
        ]
        for copy in [first] + small + w_loads:
            copy.start()
        with jax.named_scope("gather_lens"):
            first.wait()
        last = [lens_s[r] - 1 for r in range(count)]
        row_loads = [
            pltpu.make_async_copy(
                hidden.at[r * blocks + lax.div(last[r], LINES)], found.at[r], row_sem.at[r]
            )
            for r in range(count)
        ]
        for copy in row_loads:
            copy.start()
        for copy in small:
            copy.wait()
        mix = mixture(ratio_s, core, heads)
        wide = out_own[...].astype(jnp.float32)
        scale[...] = jnp.concatenate([mix[k] * wide[k : k + 1] for k in range(heads)], axis=1)
        with jax.named_scope("gather_rows"):
            for copy in row_loads:
                copy.wait()
        sub = lax.broadcasted_iota(jnp.int32, (LINES, width), 0)
        picked = jnp.zeros((LINES, width), jnp.float32)
        for r in range(count):
            block = found[r].astype(jnp.float32)
            turned = pltpu.roll(block, lax.rem(LINES + r - lax.rem(last[r], LINES), LINES), 0)
            picked = jnp.where(sub == r, turned, picked)
        lead = picked[:, :rank]
        for k in range(heads):
            at = sub[:, :rank] == count + k
            lead = jnp.where(at, jnp.broadcast_to(wide[k : k + 1], (LINES, rank)), lead)
        picked = jnp.concatenate([lead, picked[:, rank:]], axis=1)
        ends_own[...] = picked[: count + heads].astype(jnp.bfloat16)
        with jax.named_scope("gather_w"):
            for copy in w_loads:
                copy.wait()

    pl.run_scoped(
        body,
        pltpu.SemaphoreType.DMA((3,)),
        pltpu.SemaphoreType.DMA((heads,)),
        pltpu.SemaphoreType.DMA((count,)),
    )


def kernel(
    chips,
    hidden, proj, w_front, ends_own, out_own, scale, ratio, groups, lens, mask, out,
    rows_all, w_back, w_other, comb, ends, msg, slots,
    ratio_s, groups_s, lens_s, groups_v, mask_v,
    pair_recv, all_recv, here,
):
    chip, core = lax.axis_index("dp"), lax.axis_index("head")
    width = hidden.shape[2]
    count, seq = mask.shape
    heads, rank = out_own.shape
    devices = 2 * chips
    me = 2 * chip + core
    total_rows = count * seq
    everyone = groups.shape[0]
    slot = core * chips + chip
    wave = chips // WAVES
    tiles = width // TILE
    spans = [range(FRONT), range(FRONT, tiles)]
    blocks = total_rows // UNITS // TILE
    pieces = [range(FRONT), range(FRONT, tiles)]
    ahead = chip < max(1, chips // AHEAD)
    lead = chip < max(1, chips // LEAD)

    def columns(span):
        return pl.ds(span[0] * TILE, len(span) * TILE)

    def cores(act, low, high):
        def both(there, _):
            act((there, core))
            act((there, 1 - core))
            return 0

        lax.fori_loop(low, high, both, 0)

    def reader(values):
        wide = values.astype(jnp.float32)
        line = lax.broadcasted_iota(jnp.int32, (PACK, rank), 0)
        parts = [
            jnp.where(line == k, jnp.broadcast_to(wide[k : k + 1], (PACK, rank)), 0.0)
            for k in range(heads)
        ]
        return jnp.concatenate(parts, axis=1).astype(jnp.bfloat16)

    def body(sums, lines, brief, row_sem, w_sem, small_sem, pair_send, all_send):
        small = [
            pltpu.make_async_copy(ratio, ratio_s, small_sem.at[0]),
            pltpu.make_async_copy(lens, lens_s, small_sem.at[1]),
            pltpu.make_async_copy(groups, groups_s, small_sem.at[2]),
            pltpu.make_async_copy(groups, groups_v.at[0], small_sem.at[3]),
            pltpu.make_async_copy(mask, mask_v, small_sem.at[4]),
        ]
        h_loads = [
            pltpu.make_async_copy(
                hidden.at[:, :, columns(span)], rows_all.at[:, :, columns(span)], row_sem.at[d]
            )
            for d, span in enumerate(spans)
        ]
        w_loads = [
            pltpu.make_async_copy(
                proj.at[k, columns(range(FRONT, tiles))], w_back.at[:, pl.ds(k * rank, rank)],
                w_sem.at[k],
            )
            for k in range(heads)
        ]

        barrier = pltpu.get_barrier_semaphore()

        def hello(place):
            pl.semaphore_signal(barrier, inc=1, device_id=place, device_id_type=MESH)

        hello((chip, 1 - core))
        for copy in w_loads:
            copy.start()
        cores(hello, chip + 1, chips)
        for copy in h_loads + small:
            copy.start()

        def to_pair(src, dst, k):
            return pltpu.make_async_remote_copy(
                src_ref=src, dst_ref=dst, send_sem=pair_send.at[k], recv_sem=pair_recv.at[k],
                device_id=(chip, 1 - core), device_id_type=MESH,
            )

        send_ends = to_pair(ends_own, ends, 0)
        def own_piece(span):
            return w_front if span[0] < FRONT else w_back

        send_w = [
            pltpu.make_async_remote_copy(
                src_ref=own_piece(span), dst_ref=w_other.at[columns(span)],
                send_sem=pair_send.at[1 + d], recv_sem=pair_recv.at[1 + d],
                device_id=(chip, 1 - core), device_id_type=MESH,
            )
            for d, span in enumerate(pieces)
        ]

        for unit in range(UNITS):
            for ref in sums[unit] + lines[unit] + brief[unit : unit + 1]:
                pltpu.matmul_pop(ref)

        def own_tile(k):
            ref, at = (w_front, k) if k < FRONT else (w_back, k - FRONT)
            return ref[pl.ds(at * TILE, TILE), :]

        def other_tile(k):
            return w_other[pl.ds(k * TILE, TILE), :]

        def rows(unit, block, k):
            start = (unit * blocks + block) * (TILE // PACK)
            part = rows_all[pl.ds(start, TILE // PACK), :, pl.ds(k * TILE, TILE)]
            return part.reshape(TILE, TILE)

        def add_tiles(tile, span):
            for k in span:
                for unit in range(UNITS):
                    pltpu.matmul_push_rhs(tile(k), k % 2, unit)
                    for block in range(blocks):
                        pltpu.matmul_acc_lhs(
                            sums[unit][block], rows(unit, block, k), None if block else k % 2
                        )

        def add_scores(values, mix, fresh):
            lhs = reader(values)
            for block in range(blocks):
                for unit in range(UNITS):
                    inner = pltpu.matmul_pop(sums[unit][block])
                    active = jnp.tanh(inner).astype(jnp.bfloat16)
                    pltpu.matmul_push_rhs(active, block % 2, unit, transpose=True)
                    pltpu.matmul_acc_lhs(lines[unit][block], lhs, block % 2)
            for block in range(blocks):
                for unit in range(UNITS):
                    per_head = pltpu.matmul_pop(lines[unit][block])
                    line = mix[0] * per_head[0:1]
                    for k in range(1, heads):
                        line = line + mix[k] * per_head[k : k + 1]
                    at = pl.ds((unit * blocks + block) * TILE, TILE)
                    comb[:, at] = line if fresh else comb[:, at] + line

        def own_heads():
            for d, span in enumerate(spans):
                with jax.named_scope(f"wait_hidden{d}"):
                    h_loads[d].wait()
                with jax.named_scope(f"own_tiles{d}"):
                    add_tiles(own_tile, span)
            with jax.named_scope("own_scores"):
                small[0].wait()
                add_scores(out_own[...], mixture(ratio_s, core, heads), True)

        def other_heads():
            for d, span in enumerate(pieces):
                with jax.named_scope(f"wait_other{d}"):
                    send_w[d].wait_recv()
                with jax.named_scope(f"other{d}"):
                    add_tiles(other_tile, span)
            with jax.named_scope("other_scores"):
                values = ends[:, :rank].astype(jnp.float32)[count:]
                add_scores(values, mixture(ratio_s, 1 - core, heads), False)

        with jax.named_scope("wait_barrier"):
            pl.semaphore_wait(barrier, 2 * chip + 1)
        send_ends.start()

        @pl.when(ahead)
        def _():
            send_w[0].start()

        cores(
            lambda place: pl.semaphore_signal(
                here.at[lax.div(chip, wave)], inc=1, device_id=place, device_id_type=MESH
            ),
            0, chip,
        )

        turns = [range(at, at + UNITS) for at in range(0, tiles, UNITS)]

        def stage(turn):
            for unit, k in enumerate(turns[turn]):
                pltpu.matmul_push_rhs(own_tile(k), turn % 2, unit)

        lot = count + heads

        def lines_of(k, own, other):
            at = pl.ds(k * TILE, TILE)
            blank = jnp.zeros((lot, TILE), jnp.float32)
            stack = [
                ends_own[:, at].astype(jnp.float32) if own else blank,
                ends[:, at].astype(jnp.float32) if other else blank,
                jnp.zeros((PACK - 2 * lot, TILE), jnp.float32),
            ]
            return jnp.concatenate(stack, axis=0).astype(jnp.bfloat16)

        def add_lines(turn, own, other, load):
            for unit, k in enumerate(turns[turn]):
                pltpu.matmul_acc_lhs(brief[unit], lines_of(k, own, other), load)

        stage(0)
        stage(1)
        add_lines(0, True, False, 0)
        stage(2)
        with jax.named_scope("wait_w"):
            for copy in w_loads:
                copy.wait()

        @pl.when(ahead)
        def _():
            send_w[1].start()

        with jax.named_scope("wait_ends"):
            send_ends.wait_recv()
        with jax.named_scope("ends_dot"):
            add_lines(0, False, True, None)
            for turn in range(1, len(turns)):
                add_lines(turn, True, True, turn % 2)
                if turn + 2 < len(turns):
                    stage(turn + 2)
            inner = pltpu.matmul_pop(brief[0]) + pltpu.matmul_pop(brief[1])
            inner = inner[:LINES]
            active = jnp.tanh(inner).astype(jnp.bfloat16).astype(jnp.float32)
            wide = active * scale[...]
            part = sum(
                [wide[:, k * rank : (k + 1) * rank] for k in range(1, heads)], wide[:, :rank]
            )
            line = lax.broadcasted_iota(jnp.int32, (LINES, rank), 0)
            own = pltpu.roll(part, core * count, 0)
            other = pltpu.roll(part, LINES - lot + (1 - core) * count, 0)
            note = jnp.where(lax.div(line, count) == core, own, other)[: 2 * count]
            msg[...] = note
            slots[slot] = note

        def tell(place):
            pltpu.make_async_remote_copy(
                src_ref=msg, dst_ref=slots.at[slot], send_sem=all_send.at[0],
                recv_sem=all_recv, device_id=place, device_id_type=MESH,
            ).start()

        with jax.named_scope("send_lower"):
            cores(tell, 0, chip)
            tell((chip, 1 - core))

        @pl.when(ahead)
        def _():
            own_heads()

        def send_higher(k):
            low, high = jnp.maximum(k * wave, chip + 1), (k + 1) * wave

            @pl.when(low < high)
            def _():
                with jax.named_scope(f"wait_higher{k}"):
                    pl.semaphore_wait(here.at[k], 2 * (high - low))
                with jax.named_scope(f"send_higher{k}"):
                    cores(tell, low, high)

        for k in range(WAVES // 2):
            send_higher(k)

        @pl.when(lead)
        def _():
            other_heads()

        for k in range(WAVES // 2, WAVES):
            send_higher(k)

        @pl.when(jnp.logical_not(ahead))
        def _():
            for copy in send_w:
                copy.start()
            own_heads()

        @pl.when(jnp.logical_not(lead))
        def _():
            other_heads()

        for copy in small[1:]:
            copy.wait()
        send_ends.wait_send()
        for copy in send_w:
            copy.wait_send()
        rest = slots.at[pl.ds(0, devices - 1)]
        pltpu.make_async_copy(rest, rest, all_send.at[0]).wait()

    def acc(unit, size):
        return pltpu.ACC(unit)((size, TILE), jnp.float32)

    pl.run_scoped(
        body,
        [[acc(unit, TILE) for _ in range(blocks)] for unit in range(UNITS)],
        [[acc(unit, PACK) for _ in range(blocks)] for unit in range(UNITS)],
        [acc(unit, PACK) for unit in range(UNITS)],
        pltpu.SemaphoreType.DMA((2,)),
        pltpu.SemaphoreType.DMA((heads,)),
        pltpu.SemaphoreType.DMA((5,)),
        pltpu.SemaphoreType.DMA((1 + len(pieces),)),
        pltpu.SemaphoreType.DMA((1,)),
    )

    across = lax.broadcasted_iota(jnp.int32, (everyone, everyone), 1)
    down = lax.broadcasted_iota(jnp.int32, (everyone, everyone), 0)
    labels = jnp.broadcast_to(groups_v[...].astype(jnp.float32), (everyone, everyone))
    labels = jnp.sum(jnp.where(across == down, labels, 0.0), axis=1, keepdims=True)
    rollout = lax.broadcasted_iota(jnp.int32, (everyone, 1), 0)
    members = [labels == groups_s[me * count + r].astype(jnp.float32) for r in range(count)]
    owners = [rollout == me * count + r for r in range(count)]
    length = jnp.zeros((count, seq), jnp.int32)
    line = lax.broadcasted_iota(jnp.int32, (count, seq), 0)
    for r in range(count):
        length = jnp.where(line == r, lens_s[r], length)
    place = lax.broadcasted_iota(jnp.int32, (count, seq), 1)
    valid = (place < length) & (mask_v[...] == 1)
    tokens = token_weight * jnp.concatenate(
        [comb[:, pl.ds(r * seq, seq)] for r in range(count)], axis=0
    )

    rest = slots.at[pl.ds(0, devices - 1)]
    with jax.named_scope("wait_all"):
        pltpu.make_async_copy(rest, rest, all_recv).wait()

    with jax.named_scope("final"):
        total = slots[pl.ds(0, chips)] + slots[pl.ds(chips, chips)]
        reward = jnp.sum(total.reshape(everyone, rank), axis=1, keepdims=True)
        base = jnp.zeros((count, seq), jnp.float32)
        for r in range(count):
            own = jnp.sum(jnp.where(owners[r], reward, 0.0), axis=0, keepdims=True)
            mean = jnp.sum(jnp.where(members[r], reward, 0.0), axis=0, keepdims=True)
            mean = mean * (1 / GROUP)
            gap = reward - mean
            var = jnp.sum(jnp.where(members[r], gap * gap, 0.0), axis=0, keepdims=True)
            var = var * (1 / GROUP)
            best = jnp.max(jnp.where(members[r], reward, -jnp.inf), axis=0, keepdims=True)
            one = (own - mean) * lax.rsqrt(var + var_offset) - gap_weight * (best - own)
            base = jnp.where(line == r, jnp.broadcast_to(one, (count, seq)), base)
        shaped = base + tokens
        out[...] = jnp.where(valid, jnp.clip(shaped, -clip_limit, clip_limit), 0.0)


def solution(mesh):
    chips = mesh.shape["dp"]

    def on_device(hidden, head_proj, head_out, head_ratio, group_of, lengths, token_mask):
        count, seq, width = hidden.shape
        heads, _, rank = head_proj.shape
        everyone = group_of.shape[0]
        pieces = 2
        hbm = pl.BlockSpec(memory_space=pltpu.HBM)
        bf16, f32, i32 = jnp.bfloat16, jnp.float32, jnp.int32
        vmem = pl.BlockSpec(memory_space=pltpu.VMEM)
        rows = hidden.reshape(-1, PACK, width)
        early = pl.pallas_call(
            gather,
            out_shape=[
                pltpu.VMEM((FRONT * TILE, heads * rank), bf16),
                pltpu.VMEM((count + heads, width), bf16),
                pltpu.VMEM((heads, rank), bf16),
                pltpu.VMEM((1, heads * rank), f32),
            ],
            in_specs=[hbm] * 5,
            out_specs=[vmem] * 4,
            scratch_shapes=[
                pltpu.VMEM((count, LINES, width), bf16),
                pltpu.SMEM(lengths.shape, i32),
                pltpu.SMEM(head_ratio.shape, i32),
            ],
            compiler_params=pltpu.CompilerParams(vmem_limit_bytes=60 * 1024 * 1024),
            name="gather",
        )(hidden.reshape(-1, LINES, width), head_proj, head_out, head_ratio, lengths)
        early = [pltpu.with_memory_space_constraint(value, pltpu.VMEM) for value in early]
        return pl.pallas_call(
            functools.partial(kernel, chips),
            out_shape=pltpu.VMEM((count, seq), f32),
            in_specs=[hbm] * 2 + [vmem] * 4 + [hbm] * 4,
            out_specs=pl.BlockSpec(memory_space=pltpu.VMEM),
            scratch_shapes=[
                pltpu.VMEM((count * seq // PACK, PACK, width), bf16),
                pltpu.VMEM((width - FRONT * TILE, heads * rank), bf16),
                pltpu.VMEM((width, heads * rank), bf16),
                pltpu.VMEM((1, count * seq), f32),
                pltpu.VMEM((count + heads, width), bf16),
                pltpu.VMEM((2 * count, rank), f32),
                pltpu.VMEM((2 * chips, 2 * count, rank), f32),
                pltpu.SMEM(head_ratio.shape, i32),
                pltpu.SMEM(group_of.shape, i32),
                pltpu.SMEM(lengths.shape, i32),
                pltpu.VMEM((1, everyone), i32),
                pltpu.VMEM((count, seq), i32),
                pltpu.SemaphoreType.DMA((1 + pieces,)),
                pltpu.SemaphoreType.DMA,
                pltpu.SemaphoreType.REGULAR((WAVES,)),
            ],
            compiler_params=pltpu.CompilerParams(
                collective_id=0, has_side_effects=True, vmem_limit_bytes=60 * 1024 * 1024
            ),
            name="advantages",
        )(rows, head_proj, *early, head_ratio, group_of, lengths, token_mask)

    return jax.shard_map(
        on_device,
        mesh=mesh,
        in_specs=(
            P(("dp", "head"), None, None),
            P("head", None, None),
            P("head", None),
            P(),
            P(),
            P(("dp", "head")),
            P(("dp", "head"), None),
        ),
        out_specs=P(("dp", "head"), None),
        check_vma=False,
    )
```

```python
import functools

import jax
import jax.numpy as jnp
from jax import lax
from jax.experimental import pallas as pl
from jax.experimental.pallas import tpu as pltpu
from jax.sharding import PartitionSpec as P

GROUP = 16
MESH = pl.DeviceIdType.MESH

token_weight = 0.5
gap_weight = 0.5
clip_limit = 2.0
var_offset = 0.04

PACK = 16
LINES = 8
TILE = 256
UNITS = 2
AHEAD = 2
LEAD = 16
WAVES = 2
FRONT = 9


def mixture(ratio_s, part, heads):
    weights = [ratio_s[k].astype(jnp.float32) for k in range(2 * heads)]
    weight_sum = sum(weights[1:], weights[0])
    return [ratio_s[part * heads + k].astype(jnp.float32) / weight_sum for k in range(heads)]


def gather(
    hidden, proj, readout, ratio, lens, w_front, ends_own, out_own, scale,
    found, lens_s, ratio_s,
):
    core = lax.axis_index("head")
    count = found.shape[0]
    heads, width, rank = proj.shape
    blocks = hidden.shape[0] // count

    def body(sem, w_sem, row_sem):
        first = pltpu.make_async_copy(lens, lens_s, sem.at[0])
        small = [
            pltpu.make_async_copy(ratio, ratio_s, sem.at[1]),
            pltpu.make_async_copy(readout, out_own, sem.at[2]),
        ]
        w_loads = [
            pltpu.make_async_copy(
                proj.at[k, pl.ds(0, FRONT * TILE)], w_front.at[:, pl.ds(k * rank, rank)],
                w_sem.at[k],
            )
            for k in range(heads)
        ]
        for copy in [first] + small + w_loads:
            copy.start()
        with jax.named_scope("gather_lens"):
            first.wait()
        last = [lens_s[r] - 1 for r in range(count)]
        row_loads = [
            pltpu.make_async_copy(
                hidden.at[r * blocks + lax.div(last[r], LINES)], found.at[r], row_sem.at[r]
            )
            for r in range(count)
        ]
        for copy in row_loads:
            copy.start()
        for copy in small:
            copy.wait()
        mix = mixture(ratio_s, core, heads)
        wide = out_own[...].astype(jnp.float32)
        scale[...] = jnp.concatenate([mix[k] * wide[k : k + 1] for k in range(heads)], axis=1)
        with jax.named_scope("gather_rows"):
            for copy in row_loads:
                copy.wait()
        sub = lax.broadcasted_iota(jnp.int32, (LINES, width), 0)
        picked = jnp.zeros((LINES, width), jnp.float32)
        for r in range(count):
            block = found[r].astype(jnp.float32)
            turned = pltpu.roll(block, lax.rem(LINES + r - lax.rem(last[r], LINES), LINES), 0)
            picked = jnp.where(sub == r, turned, picked)
        lead = picked[:, :rank]
        for k in range(heads):
            at = sub[:, :rank] == count + k
            lead = jnp.where(at, jnp.broadcast_to(wide[k : k + 1], (LINES, rank)), lead)
        picked = jnp.concatenate([lead, picked[:, rank:]], axis=1)
        ends_own[...] = picked[: count + heads].astype(jnp.bfloat16)
        with jax.named_scope("gather_w"):
            for copy in w_loads:
                copy.wait()

    pl.run_scoped(
        body,
        pltpu.SemaphoreType.DMA((3,)),
        pltpu.SemaphoreType.DMA((heads,)),
        pltpu.SemaphoreType.DMA((count,)),
    )


def kernel(
    chips,
    hidden, proj, w_front, ends_own, out_own, scale, ratio, groups, lens, mask, out,
    rows_all, w_back, w_other, comb, ends, msg, slots,
    ratio_s, groups_s, lens_s, groups_v, mask_v,
    pair_recv, all_recv, here,
):
    chip, core = lax.axis_index("dp"), lax.axis_index("head")
    width = hidden.shape[2]
    count, seq = mask.shape
    heads, rank = out_own.shape
    devices = 2 * chips
    me = 2 * chip + core
    total_rows = count * seq
    everyone = groups.shape[0]
    slot = core * chips + chip
    wave = chips // WAVES
    tiles = width // TILE
    spans = [range(FRONT), range(FRONT, tiles)]
    blocks = total_rows // UNITS // TILE
    pieces = [range(FRONT), range(FRONT, tiles)]
    ahead = chip < max(1, chips // AHEAD)
    lead = chip < max(1, chips // LEAD)

    def columns(span):
        return pl.ds(span[0] * TILE, len(span) * TILE)

    def cores(act, low, high):
        def both(there, _):
            act((there, core))
            act((there, 1 - core))
            return 0

        lax.fori_loop(low, high, both, 0)

    def reader(values):
        wide = values.astype(jnp.float32)
        line = lax.broadcasted_iota(jnp.int32, (PACK, rank), 0)
        parts = [
            jnp.where(line == k, jnp.broadcast_to(wide[k : k + 1], (PACK, rank)), 0.0)
            for k in range(heads)
        ]
        return jnp.concatenate(parts, axis=1).astype(jnp.bfloat16)

    def body(sums, lines, brief, row_sem, w_sem, small_sem, pair_send, all_send):
        small = [
            pltpu.make_async_copy(ratio, ratio_s, small_sem.at[0]),
            pltpu.make_async_copy(lens, lens_s, small_sem.at[1]),
            pltpu.make_async_copy(groups, groups_s, small_sem.at[2]),
            pltpu.make_async_copy(groups, groups_v.at[0], small_sem.at[3]),
            pltpu.make_async_copy(mask, mask_v, small_sem.at[4]),
        ]
        h_loads = [
            pltpu.make_async_copy(
                hidden.at[:, :, columns(span)], rows_all.at[:, :, columns(span)], row_sem.at[d]
            )
            for d, span in enumerate(spans)
        ]
        w_loads = [
            pltpu.make_async_copy(
                proj.at[k, columns(range(FRONT, tiles))], w_back.at[:, pl.ds(k * rank, rank)],
                w_sem.at[k],
            )
            for k in range(heads)
        ]

        barrier = pltpu.get_barrier_semaphore()

        def hello(place):
            pl.semaphore_signal(barrier, inc=1, device_id=place, device_id_type=MESH)

        hello((chip, 1 - core))
        for copy in w_loads:
            copy.start()
        cores(hello, chip + 1, chips)
        for copy in h_loads + small:
            copy.start()

        def to_pair(src, dst, k):
            return pltpu.make_async_remote_copy(
                src_ref=src, dst_ref=dst, send_sem=pair_send.at[k], recv_sem=pair_recv.at[k],
                device_id=(chip, 1 - core), device_id_type=MESH,
            )

        send_ends = to_pair(ends_own, ends, 0)
        def own_piece(span):
            return w_front if span[0] < FRONT else w_back

        send_w = [
            pltpu.make_async_remote_copy(
                src_ref=own_piece(span), dst_ref=w_other.at[columns(span)],
                send_sem=pair_send.at[1 + d], recv_sem=pair_recv.at[1 + d],
                device_id=(chip, 1 - core), device_id_type=MESH,
            )
            for d, span in enumerate(pieces)
        ]

        for unit in range(UNITS):
            for ref in sums[unit] + lines[unit] + brief[unit : unit + 1]:
                pltpu.matmul_pop(ref)

        def own_tile(k):
            ref, at = (w_front, k) if k < FRONT else (w_back, k - FRONT)
            return ref[pl.ds(at * TILE, TILE), :]

        def other_tile(k):
            return w_other[pl.ds(k * TILE, TILE), :]

        def rows(unit, block, k):
            start = (unit * blocks + block) * (TILE // PACK)
            part = rows_all[pl.ds(start, TILE // PACK), :, pl.ds(k * TILE, TILE)]
            return part.reshape(TILE, TILE)

        def add_tiles(tile, span):
            for k in span:
                for unit in range(UNITS):
                    pltpu.matmul_push_rhs(tile(k), k % 2, unit)
                    for block in range(blocks):
                        pltpu.matmul_acc_lhs(
                            sums[unit][block], rows(unit, block, k), None if block else k % 2
                        )

        def add_scores(values, mix, fresh):
            lhs = reader(values)
            for block in range(blocks):
                for unit in range(UNITS):
                    inner = pltpu.matmul_pop(sums[unit][block])
                    active = jnp.tanh(inner).astype(jnp.bfloat16)
                    pltpu.matmul_push_rhs(active, block % 2, unit, transpose=True)
                    pltpu.matmul_acc_lhs(lines[unit][block], lhs, block % 2)
            for block in range(blocks):
                for unit in range(UNITS):
                    per_head = pltpu.matmul_pop(lines[unit][block])
                    line = mix[0] * per_head[0:1]
                    for k in range(1, heads):
                        line = line + mix[k] * per_head[k : k + 1]
                    at = pl.ds((unit * blocks + block) * TILE, TILE)
                    comb[:, at] = line if fresh else comb[:, at] + line

        def own_heads():
            for d, span in enumerate(spans):
                with jax.named_scope(f"wait_hidden{d}"):
                    h_loads[d].wait()
                with jax.named_scope(f"own_tiles{d}"):
                    add_tiles(own_tile, span)
            with jax.named_scope("own_scores"):
                small[0].wait()
                add_scores(out_own[...], mixture(ratio_s, core, heads), True)

        def other_heads():
            for d, span in enumerate(pieces):
                with jax.named_scope(f"wait_other{d}"):
                    send_w[d].wait_recv()
                with jax.named_scope(f"other{d}"):
                    add_tiles(other_tile, span)
            with jax.named_scope("other_scores"):
                values = ends[:, :rank].astype(jnp.float32)[count:]
                add_scores(values, mixture(ratio_s, 1 - core, heads), False)

        with jax.named_scope("wait_barrier"):
            pl.semaphore_wait(barrier, 2 * chip + 1)
        send_ends.start()

        @pl.when(ahead)
        def _():
            send_w[0].start()

        cores(
            lambda place: pl.semaphore_signal(
                here.at[lax.div(chip, wave)], inc=1, device_id=place, device_id_type=MESH
            ),
            0, chip,
        )

        turns = [range(at, at + UNITS) for at in range(0, tiles, UNITS)]

        def stage(turn):
            for unit, k in enumerate(turns[turn]):
                pltpu.matmul_push_rhs(own_tile(k), turn % 2, unit)

        lot = count + heads

        def lines_of(k, own, other):
            at = pl.ds(k * TILE, TILE)
            blank = jnp.zeros((lot, TILE), jnp.float32)
            stack = [
                ends_own[:, at].astype(jnp.float32) if own else blank,
                ends[:, at].astype(jnp.float32) if other else blank,
                jnp.zeros((PACK - 2 * lot, TILE), jnp.float32),
            ]
            return jnp.concatenate(stack, axis=0).astype(jnp.bfloat16)

        def add_lines(turn, own, other, load):
            for unit, k in enumerate(turns[turn]):
                pltpu.matmul_acc_lhs(brief[unit], lines_of(k, own, other), load)

        stage(0)
        stage(1)
        add_lines(0, True, False, 0)
        stage(2)
        with jax.named_scope("wait_w"):
            for copy in w_loads:
                copy.wait()

        @pl.when(ahead)
        def _():
            send_w[1].start()

        with jax.named_scope("wait_ends"):
            send_ends.wait_recv()
        with jax.named_scope("ends_dot"):
            add_lines(0, False, True, None)
            for turn in range(1, len(turns)):
                add_lines(turn, True, True, turn % 2)
                if turn + 2 < len(turns):
                    stage(turn + 2)
            inner = pltpu.matmul_pop(brief[0]) + pltpu.matmul_pop(brief[1])
            inner = inner[:LINES]
            active = jnp.tanh(inner).astype(jnp.bfloat16).astype(jnp.float32)
            wide = active * scale[...]
            part = sum(
                [wide[:, k * rank : (k + 1) * rank] for k in range(1, heads)], wide[:, :rank]
            )
            line = lax.broadcasted_iota(jnp.int32, (LINES, rank), 0)
            own = pltpu.roll(part, core * count, 0)
            other = pltpu.roll(part, LINES - lot + (1 - core) * count, 0)
            note = jnp.where(lax.div(line, count) == core, own, other)[: 2 * count]
            msg[...] = note
            slots[slot] = note

        def tell(place):
            pltpu.make_async_remote_copy(
                src_ref=msg, dst_ref=slots.at[slot], send_sem=all_send.at[0],
                recv_sem=all_recv, device_id=place, device_id_type=MESH,
            ).start()

        with jax.named_scope("send_lower"):
            @pl.when(chip > 0)
            def _():
                tell((0, core))
                tell((0, 1 - core))

            cores(tell, 1, chip)
            tell((chip, 1 - core))

        @pl.when(ahead)
        def _():
            own_heads()

        def send_higher(k):
            low, high = jnp.maximum(k * wave, chip + 1), (k + 1) * wave

            @pl.when(low < high)
            def _():
                with jax.named_scope(f"wait_higher{k}"):
                    pl.semaphore_wait(here.at[k], 2 * (high - low))
                with jax.named_scope(f"send_higher{k}"):
                    cores(tell, low, high)

        for k in range(WAVES // 2):
            send_higher(k)

        @pl.when(lead)
        def _():
            other_heads()

        for k in range(WAVES // 2, WAVES):
            send_higher(k)

        @pl.when(jnp.logical_not(ahead))
        def _():
            for copy in send_w:
                copy.start()
            own_heads()

        @pl.when(jnp.logical_not(lead))
        def _():
            other_heads()

        for copy in small[1:]:
            copy.wait()
        send_ends.wait_send()
        for copy in send_w:
            copy.wait_send()
        rest = slots.at[pl.ds(0, devices - 1)]
        pltpu.make_async_copy(rest, rest, all_send.at[0]).wait()

    def acc(unit, size):
        return pltpu.ACC(unit)((size, TILE), jnp.float32)

    pl.run_scoped(
        body,
        [[acc(unit, TILE) for _ in range(blocks)] for unit in range(UNITS)],
        [[acc(unit, PACK) for _ in range(blocks)] for unit in range(UNITS)],
        [acc(unit, PACK) for unit in range(UNITS)],
        pltpu.SemaphoreType.DMA((2,)),
        pltpu.SemaphoreType.DMA((heads,)),
        pltpu.SemaphoreType.DMA((5,)),
        pltpu.SemaphoreType.DMA((1 + len(pieces),)),
        pltpu.SemaphoreType.DMA((1,)),
    )

    across = lax.broadcasted_iota(jnp.int32, (everyone, everyone), 1)
    down = lax.broadcasted_iota(jnp.int32, (everyone, everyone), 0)
    labels = jnp.broadcast_to(groups_v[...].astype(jnp.float32), (everyone, everyone))
    labels = jnp.sum(jnp.where(across == down, labels, 0.0), axis=1, keepdims=True)
    rollout = lax.broadcasted_iota(jnp.int32, (everyone, 1), 0)
    members = [labels == groups_s[me * count + r].astype(jnp.float32) for r in range(count)]
    owners = [rollout == me * count + r for r in range(count)]
    length = jnp.zeros((count, seq), jnp.int32)
    line = lax.broadcasted_iota(jnp.int32, (count, seq), 0)
    for r in range(count):
        length = jnp.where(line == r, lens_s[r], length)
    place = lax.broadcasted_iota(jnp.int32, (count, seq), 1)
    valid = (place < length) & (mask_v[...] == 1)
    tokens = token_weight * jnp.concatenate(
        [comb[:, pl.ds(r * seq, seq)] for r in range(count)], axis=0
    )

    rest = slots.at[pl.ds(0, devices - 1)]
    with jax.named_scope("wait_all"):
        pltpu.make_async_copy(rest, rest, all_recv).wait()

    with jax.named_scope("final"):
        total = slots[pl.ds(0, chips)] + slots[pl.ds(chips, chips)]
        reward = jnp.sum(total.reshape(everyone, rank), axis=1, keepdims=True)
        base = jnp.zeros((count, seq), jnp.float32)
        for r in range(count):
            own = jnp.sum(jnp.where(owners[r], reward, 0.0), axis=0, keepdims=True)
            mean = jnp.sum(jnp.where(members[r], reward, 0.0), axis=0, keepdims=True)
            mean = mean * (1 / GROUP)
            gap = reward - mean
            var = jnp.sum(jnp.where(members[r], gap * gap, 0.0), axis=0, keepdims=True)
            var = var * (1 / GROUP)
            best = jnp.max(jnp.where(members[r], reward, -jnp.inf), axis=0, keepdims=True)
            one = (own - mean) * lax.rsqrt(var + var_offset) - gap_weight * (best - own)
            base = jnp.where(line == r, jnp.broadcast_to(one, (count, seq)), base)
        shaped = base + tokens
        out[...] = jnp.where(valid, jnp.clip(shaped, -clip_limit, clip_limit), 0.0)


def solution(mesh):
    chips = mesh.shape["dp"]

    def on_device(hidden, head_proj, head_out, head_ratio, group_of, lengths, token_mask):
        count, seq, width = hidden.shape
        heads, _, rank = head_proj.shape
        everyone = group_of.shape[0]
        pieces = 2
        hbm = pl.BlockSpec(memory_space=pltpu.HBM)
        bf16, f32, i32 = jnp.bfloat16, jnp.float32, jnp.int32
        vmem = pl.BlockSpec(memory_space=pltpu.VMEM)
        rows = hidden.reshape(-1, PACK, width)
        early = pl.pallas_call(
            gather,
            out_shape=[
                pltpu.VMEM((FRONT * TILE, heads * rank), bf16),
                pltpu.VMEM((count + heads, width), bf16),
                pltpu.VMEM((heads, rank), bf16),
                pltpu.VMEM((1, heads * rank), f32),
            ],
            in_specs=[hbm] * 5,
            out_specs=[vmem] * 4,
            scratch_shapes=[
                pltpu.VMEM((count, LINES, width), bf16),
                pltpu.SMEM(lengths.shape, i32),
                pltpu.SMEM(head_ratio.shape, i32),
            ],
            compiler_params=pltpu.CompilerParams(vmem_limit_bytes=60 * 1024 * 1024),
            name="gather",
        )(hidden.reshape(-1, LINES, width), head_proj, head_out, head_ratio, lengths)
        early = [pltpu.with_memory_space_constraint(value, pltpu.VMEM) for value in early]
        return pl.pallas_call(
            functools.partial(kernel, chips),
            out_shape=pltpu.VMEM((count, seq), f32),
            in_specs=[hbm] * 2 + [vmem] * 4 + [hbm] * 4,
            out_specs=pl.BlockSpec(memory_space=pltpu.VMEM),
            scratch_shapes=[
                pltpu.VMEM((count * seq // PACK, PACK, width), bf16),
                pltpu.VMEM((width - FRONT * TILE, heads * rank), bf16),
                pltpu.VMEM((width, heads * rank), bf16),
                pltpu.VMEM((1, count * seq), f32),
                pltpu.VMEM((count + heads, width), bf16),
                pltpu.VMEM((2 * count, rank), f32),
                pltpu.VMEM((2 * chips, 2 * count, rank), f32),
                pltpu.SMEM(head_ratio.shape, i32),
                pltpu.SMEM(group_of.shape, i32),
                pltpu.SMEM(lengths.shape, i32),
                pltpu.VMEM((1, everyone), i32),
                pltpu.VMEM((count, seq), i32),
                pltpu.SemaphoreType.DMA((1 + pieces,)),
                pltpu.SemaphoreType.DMA,
                pltpu.SemaphoreType.REGULAR((WAVES,)),
            ],
            compiler_params=pltpu.CompilerParams(
                collective_id=0, has_side_effects=True, vmem_limit_bytes=60 * 1024 * 1024
            ),
            name="advantages",
        )(rows, head_proj, *early, head_ratio, group_of, lengths, token_mask)

    return jax.shard_map(
        on_device,
        mesh=mesh,
        in_specs=(
            P(("dp", "head"), None, None),
            P("head", None, None),
            P("head", None),
            P(),
            P(),
            P(("dp", "head")),
            P(("dp", "head"), None),
        ),
        out_specs=P(("dp", "head"), None),
        check_vma=False,
    )
```
